32 devices in a mesh: row: 8 (over z, core), col: 4 (over y, x).
Axes of the slice: x: 2, y: 2, z: 4, core: 2. Of those that a mesh axis runs over, the one named last changes fastest.
Arguments:
- fine_residual: float32 [16, 3, 1572864], P(None, None, ('row', 'col')), may hold values from -6 to 6
- restriction: float32 [3, 3, 1572864], P(None, None, ('row', 'col')), may hold values from -1.25 to 1.25
- restriction_pattern: int32 [1572864], P(('row', 'col')), may hold values 0 or 1
- cell_aggregate: int32 [384, 512], P('row', 'col'), may hold values from 0 to 196607, as said below
- block_inverse: float32 [3, 3, 384, 512], P(None, None, 'row', 'col'), may hold values from -4 to 4, as said below
- off_blocks: float32 [4, 3, 3, 384, 512], P(None, None, None, 'row', 'col'), may hold values from -0.5 to 0.5
- operator_pattern: int32 [4, 384, 512], P(None, 'row', 'col'), may hold values 0 or 1
Outputs:
- coarse_solution: float32 [16, 3, 384, 512], P(None, None, 'row', 'col')
- fine_correction: float32 [16, 3, 1572864], P(None, None, ('row', 'col'))
The draws below stay inside these ranges and needn't reach their ends.
Inputs may be any that keep to these rules, and one draw needn't show every extreme that they name: `cell_aggregate`: every aggregate number 0 to 196607 stands in exactly one coarse cell. Aggregate g = f * 6144 + a lies in the tile numbered a mod 32, where the tile of rows i * 48 to (i + 1) * 48 - 1 and columns j * 128 to (j + 1) * 128 - 1 is numbered i * 4 + j. `block_inverse`: each 3x3 block is the inverse of a cell's diagonal block.
All inputs are finite; a program needn't handle non-finite values. No bound on the sum of `restriction_pattern` or of `operator_pattern` on one device may be relied on, other than what follows from the above.
Results may differ from the reference program's by a relative error of at most 0.00002.
Values sent between devices are 32-bit elements; how exact they have to be, the bound alone decides.
A program may use at most 128 MiB of HBM per device.

```python
import jax
import jax.numpy as jnp

NRHS = 16
CR = 48
CC = 128
FPA = 8
ITERS = 4
AGG_DEV = 6144
FINE = 1572864
NCR = 384
NCC = 512
N_ROW = 8
N_COL = 4


def draw_cell_aggregate(key, part):
    devices = N_ROW * N_COL

    def tile_cells(tile):
        order = jax.random.permutation(jax.random.fold_in(key, tile), AGG_DEV)
        owner = order % devices
        local = order // devices * devices + tile
        return (owner * AGG_DEV + local).astype(jnp.int32)
    tiles = jax.vmap(tile_cells)(jnp.arange(devices, dtype=jnp.int32))
    grid = tiles.reshape(N_ROW, N_COL, CR, CC).transpose(0, 2, 1, 3)
    return grid.reshape(N_ROW * CR, N_COL * CC)


def draw_block_inverse(key, part):
    scale_key = jax.random.fold_in(key, 11)
    noise_key = jax.random.fold_in(key, 12)
    scale = jnp.exp(jax.random.uniform(scale_key, (NCR, NCC), jnp.float32, jnp.log(0.5), jnp.log(2.0)))
    noise = 0.3 * jnp.clip(jax.random.normal(noise_key, (3, 3, NCR, NCC), jnp.float32), -2.5, 2.5)
    identity = jnp.eye(3, dtype=jnp.float32)[:, :, None, None]
    return (scale[None, None] * (identity + noise)).astype(jnp.float32)


def touch_ends(result, rng, low, high):
    shape = result.shape
    place = [jax.random.randint(jax.random.fold_in(rng, axis), (), 0, shape[axis]) for axis in range(len(shape))]
    result = result.at[tuple(place)].set(low)
    longest = shape.index(max(shape))
    place[longest] = (place[longest] + 1) % shape[longest]
    return result.at[tuple(place)].set(high)


def block_scale(rng, dims, split, smallest, high):
    def one(dim, parts):
        heights = jax.random.uniform(jax.random.fold_in(jax.random.fold_in(rng, 6), dim), (parts,), jnp.float32, smallest / len(split), high / len(split))
        return jnp.repeat(jnp.exp(heights), dims[dim] // parts).reshape((-1,) + (1,) * (len(dims) - dim - 1))

    level = one(*split[0])
    for cut in split[1:]:
        level = level * one(*cut)
    return level


def centred(stream_key, extent, width, bound, pieces=(), kind=jnp.bfloat16):
    drawn = width * jax.random.normal(stream_key, extent, jnp.float32)
    if pieces:
        drawn = drawn * block_scale(stream_key, extent, pieces, -0.22, 0.18)
    return jnp.clip(drawn, -bound, bound).astype(kind)


def setup_inputs(seed: int = 0) -> dict:
    key_list = jax.random.split(jax.random.key(seed), 8)
    return {
        "fine_residual": centred(key_list[0], (NRHS, 3, FINE), 1.0, 6.0, ((2, 32),), jnp.float32),
        "restriction": centred(key_list[1], (3, 3, FINE), (3 * FPA) ** -0.5, 1.25, ((2, 32),), jnp.float32),
        "restriction_pattern": touch_ends((jax.random.randint(key_list[2], (FINE,), 0, 4) < 3).astype(jnp.int32), jax.random.fold_in(key_list[2], 1), 0, 1),
        "cell_aggregate": draw_cell_aggregate(jax.random.fold_in(key_list[7], 71), 0),
        "block_inverse": draw_block_inverse(jax.random.fold_in(key_list[7], 71), 0),
        "off_blocks": centred(key_list[5], (4, 3, 3, NCR, NCC), 0.1, 0.5, ((3, 8), (4, 4)), jnp.float32),
        "operator_pattern": touch_ends((jax.random.randint(key_list[6], (4, NCR, NCC), 0, 4) < 3).astype(jnp.int32), jax.random.fold_in(key_list[6], 1), 0, 1),
    }


def apply_inverse(inverse, vector):
    total = inverse[:, 0][None] * vector[:, 0][:, None]
    for source in range(1, 3):
        total = total + inverse[:, source][None] * vector[:, source][:, None]
    return total


def neighbours(padded):
    height = padded.shape[-2] - 2
    breadth = padded.shape[-1] - 2
    return (padded[..., 0:height, 1:breadth + 1], padded[..., 2:height + 2, 1:breadth + 1],
            padded[..., 1:height + 1, 0:breadth], padded[..., 1:height + 1, 2:breadth + 2])


def sweep_once(padded, target_side, inverse, coupling):
    total = target_side
    for direction, shifted in enumerate(neighbours(padded)):
        for source in range(3):
            total = total - coupling[direction, :, source][None] * shifted[:, source][:, None]
    return apply_inverse(inverse, total)


def restrict_terms(residual, restriction, pattern):
    masked = residual * pattern.astype(jnp.float32)[None, None]
    total = restriction[:, 0][None] * masked[:, 0][:, None]
    for source in range(1, 3):
        total = total + restriction[:, source][None] * masked[:, source][:, None]
    loads = total.shape[0]
    return total.reshape(loads, 3, -1, FPA, AGG_DEV).sum(axis=3).reshape(loads, 3, -1)


def prolong_terms(values, restriction, pattern):
    loads = values.shape[0]
    slabs = values.shape[2] // AGG_DEV
    expanded = jnp.broadcast_to(values.reshape(loads, 3, slabs, 1, AGG_DEV), (loads, 3, slabs, FPA, AGG_DEV)).reshape(loads, 3, -1)
    total = restriction[0][None] * expanded[:, 0][:, None]
    for source in range(1, 3):
        total = total + restriction[source][None] * expanded[:, source][:, None]
    return total * pattern.astype(jnp.float32)[None, None]


def reference(fine_residual, restriction, restriction_pattern, cell_aggregate, block_inverse, off_blocks, operator_pattern):
    loads = fine_residual.shape[0]
    aggregate_rhs = restrict_terms(fine_residual, restriction, restriction_pattern)
    flat_cells = cell_aggregate.reshape(-1)
    coarse_rhs = jnp.take(aggregate_rhs, flat_cells, axis=2).reshape(loads, 3, NCR, NCC)
    coupling = off_blocks * operator_pattern.astype(jnp.float32)[:, None, None]
    iterate = apply_inverse(block_inverse, coarse_rhs)
    for sweep_index in range(ITERS - 1):
        padded = jnp.pad(iterate, ((0, 0), (0, 0), (1, 1), (1, 1)))
        iterate = sweep_once(padded, coarse_rhs, block_inverse, coupling)
    aggregate_solution = jnp.zeros_like(aggregate_rhs).at[:, :, flat_cells].set(iterate.reshape(loads, 3, -1))
    fine_correction = prolong_terms(aggregate_solution, restriction, restriction_pattern)
    return iterate, fine_correction
```

```python
import functools

import jax
import jax.numpy as jnp
from jax import lax
from jax.experimental import pallas as pl
from jax.experimental.pallas import tpu as pltpu
from jax.sharding import PartitionSpec as P

FPA = 8
ITERS = 4
AGG_DEV = 6144
LANES = 128
GROUP = 8
PAIR = 2
HALVES = 2
SLOT_REFS = 6
UNROLL = 16
MESH = pl.DeviceIdType.MESH
VMEM_LIMIT = 56 * 1024 * 1024


def spec_vmem():
    return pl.BlockSpec(memory_space=pltpu.VMEM)


def spec_any():
    return pl.BlockSpec(memory_space=pl.ANY)


def peer_of(me, index, devices, col_count):
    peer = lax.rem(me + 13 * index, devices)
    return peer, {"row": peer // col_count, "col": lax.rem(peer, col_count)}


def greet(devices, col_count, me):
    barrier = pltpu.get_barrier_semaphore()

    def signal(index, carry):
        _, where = peer_of(me, index, devices, col_count)
        pl.semaphore_signal(barrier, inc=1, device_id=where, device_id_type=MESH)
        return carry

    lax.fori_loop(1, devices, signal, 0)
    return barrier


def tables_kernel(devices, cells_ref, slots_ref, inverse_ref):
    height = cells_ref.shape[0]
    parts = LANES // devices
    blocks = AGG_DEV // LANES
    piece = blocks * parts // GROUP
    value = cells_ref[...].astype(jnp.float32)
    owner = jnp.floor((value + 0.5) * (1.0 / AGG_DEV))
    inside = value - owner * AGG_DEV
    block = jnp.floor((inside + 0.5) * (1.0 / LANES))
    part = jnp.floor((inside - block * LANES + 0.5) * (1.0 / devices))
    group = jnp.floor((block + 0.5) * (1.0 / GROUP))
    slot = owner * (GROUP * piece) + (block - group * GROUP) * piece + group * parts + part
    slots_ref[...] = slot.astype(jnp.int32)
    place = part * devices + owner
    rows = lax.broadcasted_iota(jnp.int32, (blocks, LANES), 0).astype(jnp.float32)
    lanes = lax.broadcasted_iota(jnp.int32, (blocks, LANES), 1).astype(jnp.float32)
    places = lax.broadcasted_iota(jnp.int32, (LANES, LANES), 0).astype(jnp.float32)
    total = jnp.zeros((2 * blocks, LANES), jnp.float32)
    for r in range(height):
        hit = rows == block[r : r + 1, :]
        low = jnp.where(hit, lanes, 0.0)
        high = jnp.where(hit, float(r), 0.0)
        left = jnp.concatenate([low, high], axis=0).astype(jnp.bfloat16)
        right = jnp.where(places == place[r : r + 1, :], 1.0, 0.0).astype(jnp.bfloat16)
        total = total + lax.dot_general(left, right, (((1,), (1,)), ((), ())), preferred_element_type=jnp.float32)
    inverse_ref[...] = (total[:blocks] + total[blocks:] * LANES).astype(jnp.int32)


def tables(cells, devices):
    blocks = AGG_DEV // LANES
    slots, inverse = pl.pallas_call(
        functools.partial(tables_kernel, devices),
        in_specs=[spec_vmem()],
        out_specs=(spec_vmem(), spec_vmem()),
        out_shape=(
            jax.ShapeDtypeStruct(cells.shape, jnp.int32),
            jax.ShapeDtypeStruct((blocks, LANES), jnp.int32),
        ),
        name="tables",
    )(cells)
    return slots.reshape(-1), inverse.reshape(-1)


def main_kernel(row_count, col_count, loads, *refs):
    (
        slots_hbm,
        places_hbm,
        residual_hbm,
        restriction_hbm,
        present_hbm,
        inverse_hbm,
        blocks_hbm,
        pattern_hbm,
        arrived,
        planes_hbm,
    ) = refs[:10]
    slots = refs[10 : 10 + SLOT_REFS]
    (
        places,
        residual,
        restriction,
        present_all,
        inverse_ref,
        blocks_ref,
        pattern_ref,
        stage,
        sent,
        chunk,
        table,
        ordered,
        rhs,
        planes_ref,
        base,
        x,
        mixed,
        edge,
        halo,
        packed,
        residual_sem,
        restriction_sem,
        small_sem,
        slots_sem,
        send_sem,
        recv_sem,
        halo_send_sem,
        halo_recv_sem,
        back_send_sem,
        back_recv_sem,
        own_sem,
    ) = refs[10 + SLOT_REFS :]
    devices = row_count * col_count
    parts = LANES // devices
    pairs = residual.shape[0]
    width = residual.shape[-1]
    height = inverse_ref.shape[2]
    few = PAIR * parts
    piece = pairs * few
    row = lax.axis_index("row")
    col = lax.axis_index("col")
    me = row * col_count + col
    barrier = greet(devices, col_count, me)

    small = [
        pltpu.make_async_copy(present_hbm, present_all, small_sem.at[0]),
        pltpu.make_async_copy(inverse_hbm, inverse_ref, small_sem.at[1]),
        pltpu.make_async_copy(blocks_hbm, blocks_ref, small_sem.at[2]),
        pltpu.make_async_copy(pattern_hbm, pattern_ref, small_sem.at[3]),
        pltpu.make_async_copy(places_hbm, places, small_sem.at[4]),
    ]
    span = slots[0].shape[0]
    for n in range(SLOT_REFS):
        small.append(pltpu.make_async_copy(slots_hbm.at[pl.ds(n * span, span)], slots[n], slots_sem.at[n]))
    small[0].start()
    for pair in range(pairs):
        for p in range(FPA):
            lanes = pl.ds((p * pairs + pair) * width, width)
            pltpu.make_async_copy(residual_hbm.at[:, :, lanes], residual.at[pair, p], residual_sem.at[pair]).start()
            pltpu.make_async_copy(restriction_hbm.at[:, :, lanes], restriction.at[pair, p], restriction_sem.at[pair]).start()
    for copy in small[1:]:
        copy.start()
    halo[...] = jnp.zeros_like(halo)
    small[0].wait()

    def send_first(pair):
        def send(index, carry):
            peer, where = peer_of(me, index, devices, col_count)
            pltpu.make_async_remote_copy(
                src_ref=sent.at[pair, peer],
                dst_ref=chunk.at[pair, me],
                send_sem=send_sem,
                recv_sem=recv_sem,
                device_id=where,
                device_id_type=MESH,
            ).start()
            return carry

        lax.fori_loop(1, devices, send, 0)

    def restrict(pair):
        pltpu.make_async_copy(residual.at[pair], residual.at[pair], residual_sem.at[pair]).wait()
        pltpu.make_async_copy(restriction.at[pair], restriction.at[pair], restriction_sem.at[pair]).wait()
        for half in range(PAIR):
            for block in range(GROUP):
                start = (half * GROUP + block) * LANES
                lanes = slice(start, start + LANES)
                which = half * GROUP + block
                totals = [None, None, None]
                for p in range(FPA):
                    present = present_all[p * pairs + pair, which : which + 1, :].astype(jnp.float32)
                    for j in range(3):
                        masked = residual[pair, p, j, :, lanes] * present
                        for i in range(3):
                            term = restriction[pair, p, i, j : j + 1, lanes] * masked
                            totals[i] = term if totals[i] is None else totals[i] + term
                for i in range(3):
                    stage[i, block * loads : (block + 1) * loads, :] = totals[i]
            for i in range(3):
                turned = stage[i].T
                for part in range(parts):
                    sent[pair, :, (i * PAIR + half) * parts + part, :] = turned[part * devices : (part + 1) * devices, :]

    restrict(0)
    pl.semaphore_wait(barrier, devices - 1)
    send_first(0)

    def later(pair, carry):
        restrict(pair)
        send_first(pair)
        return carry

    lax.fori_loop(1, pairs, later, 0)
    for copy in small[1:]:
        copy.wait()

    def keep(pair, carry):
        chunk[pair, me] = sent[pair, me]
        return carry

    lax.fori_loop(0, pairs, keep, 0)

    def fold(d, carry):
        on = pattern_ref[d].astype(jnp.float32)
        for k in range(3):
            column = [blocks_ref[d, j, k] * on for j in range(3)]
            for i in range(3):
                total = inverse_ref[i, 0] * column[0]
                total = total + inverse_ref[i, 1] * column[1]
                mixed[d, i, k] = total + inverse_ref[i, 2] * column[2]
        return carry

    lax.fori_loop(0, 4, fold, 0)
    _, where = peer_of(me, 1, devices, col_count)
    every = pltpu.make_async_remote_copy(
        src_ref=sent.at[:, pl.ds(0, devices - 1)],
        dst_ref=chunk.at[:, pl.ds(0, devices - 1)],
        send_sem=send_sem,
        recv_sem=recv_sem,
        device_id=where,
        device_id_type=MESH,
    )
    every.wait_send()
    every.wait_recv()

    lane_few = lax.broadcasted_iota(jnp.int32, (few, LANES), 1) // loads

    def unpack(f, carry):
        for pair in range(pairs):
            parts_i = [chunk[pair, f, i * few : (i + 1) * few, :] for i in range(3)]
            moved = [parts_i[0], pltpu.roll(parts_i[1], loads, 1), pltpu.roll(parts_i[2], 2 * loads, 1)]
            for group in ((0, 3), (1, 4), (2, 5), (6,), (7,)):
                second = functools.reduce(jnp.logical_or, [lane_few == (b + 1) % GROUP for b in group])
                third = functools.reduce(jnp.logical_or, [lane_few == (b + 2) % GROUP for b in group])
                mix = jnp.where(third, moved[2], jnp.where(second, moved[1], moved[0]))
                for b in group:
                    line = pltpu.roll(mix, (LANES - b * loads) % LANES, 1) if b else mix
                    table[pl.ds(f * (GROUP * piece) + b * piece + pair * few, few), :] = line
        return carry

    lax.fori_loop(0, devices, unpack, 0, unroll=2)

    def take(r, carry):
        at = pl.multiple_of(r * UNROLL, UNROLL)
        for j in range(UNROLL):
            for n in range(SLOT_REFS):
                ordered[pl.ds(n * span + at + j, 1), :] = table[pl.ds(slots[n][at + j], 1), :]
        return carry

    lax.fori_loop(0, span // UNROLL, take, 0)

    def turn(r, carry):
        turned = ordered[pl.ds(pl.multiple_of(r * LANES, LANES), LANES), :].T
        rhs[pl.ds(r, 3 * loads, stride=height), :] = turned[: 3 * loads, :]
        return carry

    lax.fori_loop(0, height, turn, 0, unroll=4)

    part_loads = loads // HALVES
    planes = 3 * part_loads
    exists = (row > 0, row < row_count - 1, col > 0, col < col_count - 1)
    peers = (
        {"row": row - 1, "col": col},
        {"row": row + 1, "col": col},
        {"row": row, "col": col - 1},
        {"row": row, "col": col + 1},
    )
    extent = (planes, planes, height, height)
    lane = lax.broadcasted_iota(jnp.int32, (height, LANES), 1)

    def plane_rows(index):
        return pl.ds(pl.multiple_of(index * height, height), height)

    def first(half):
        def one(q, carry):
            source = half * part_loads + q
            given = [rhs[plane_rows(j * loads + source), :] for j in range(3)]
            for i in range(3):
                total = inverse_ref[i, 0] * given[0]
                total = total + inverse_ref[i, 1] * given[1]
                total = total + inverse_ref[i, 2] * given[2]
                base[half * planes + i * part_loads + q] = total
                x[0, half * planes + i * part_loads + q, 8 : 8 + height, :] = total
            return carry

        lax.fori_loop(0, part_loads, one, 0)

    def pack(slot, step, half):
        own = slice(half * planes, (half + 1) * planes)
        edge[step, half, 0, :planes, :] = x[slot, own, 8, :]
        edge[step, half, 1, :planes, :] = x[slot, own, 7 + height, :]

        def columns(p, carry):
            left, right = carry
            plane = x[slot, half * planes + p, 8 : 8 + height, :]
            left = jnp.where(lane == p, pltpu.roll(plane, p, 1), left)
            right = jnp.where(lane == p, pltpu.roll(plane, p + 1, 1), right)
            return left, right

        blank = jnp.zeros((height, LANES), jnp.float32)
        left, right = lax.fori_loop(0, planes, columns, (blank, blank), unroll=4)
        edge[step, half, 2, :height, :] = left
        edge[step, half, 3, :height, :] = right

    def copy_edge(step, half, d, side):
        return pltpu.make_async_remote_copy(
            src_ref=edge.at[step, half, d, pl.ds(0, extent[d])],
            dst_ref=halo.at[step, half, side, pl.ds(0, extent[d])],
            send_sem=halo_send_sem.at[step, half, d],
            recv_sem=halo_recv_sem.at[step, half, side],
            device_id=peers[d],
            device_id_type=MESH,
        )

    def start(step, half):
        for d in range(4):

            @pl.when(exists[d])
            def _():
                copy_edge(step, half, d, d ^ 1).start()

    for half in range(HALVES):
        first(half)
        pack(0, 0, half)
        start(0, half)
    for step in range(ITERS - 1):
        old = step % 2
        last = step == ITERS - 2
        for half in range(HALVES):
            for d in range(4):

                @pl.when(exists[d])
                def _():
                    copy_edge(step, half, d, d).wait_send()
                    copy_edge(step, half, d, d).wait_recv()

            own = slice(half * planes, (half + 1) * planes)
            x[old, own, 7, :] = halo[step, half, 0, :planes, :]
            x[old, own, 8 + height, :] = halo[step, half, 1, :planes, :]

            def update(q, carry):
                totals = [base[half * planes + i * part_loads + q] for i in range(3)]
                for k in range(3):
                    local = k * part_loads + q
                    p = half * planes + local
                    plane = x[old, p, 8 : 8 + height, :]
                    left = jnp.where(
                        lane == 0,
                        pltpu.roll(halo[step, half, 2, :height, :], lax.rem(LANES - local, LANES), 1),
                        pltpu.roll(plane, 1, 1),
                    )
                    right = jnp.where(
                        lane == LANES - 1,
                        pltpu.roll(halo[step, half, 3, :height, :], LANES - 1 - local, 1),
                        pltpu.roll(plane, LANES - 1, 1),
                    )
                    shifted = (x[old, p, 7 : 7 + height, :], x[old, p, 9 : 9 + height, :], left, right)
                    for d in range(4):
                        for i in range(3):
                            totals[i] = totals[i] - mixed[d, i, k] * shifted[d]
                for i in range(3):
                    if last:
                        planes_ref[plane_rows(i * loads + half * part_loads + q), :] = totals[i]
                    else:
                        x[1 - old, half * planes + i * part_loads + q, 8 : 8 + height, :] = totals[i]
                return carry

            lax.fori_loop(0, part_loads, update, 0)
            if not last:
                pack(1 - old, step + 1, half)
                start(step + 1, half)

    out_copy = pltpu.make_async_copy(planes_ref, planes_hbm, small_sem.at[0])
    out_copy.start()

    def back(r, carry):
        plane = planes_ref[pl.ds(r, 3 * loads, stride=height), :]
        ordered[pl.ds(pl.multiple_of(r * LANES, LANES), LANES), : 3 * loads] = plane.T
        return carry

    lax.fori_loop(0, height, back, 0, unroll=4)
    lane_piece = lax.broadcasted_iota(jnp.int32, (piece, LANES), 1)

    def gather_piece(f):
        for block in range(GROUP):
            for n in range(piece):
                where = ((n // parts) * GROUP + block) * LANES + (n % parts) * devices
                table[pl.ds(block * piece + n, 1), :] = ordered[pl.ds(places[f + where], 1), :]

    def pack_piece(f):
        gather_piece(f)
        lines = [table[block * piece : (block + 1) * piece, :] for block in range(GROUP)]
        for i in range(3):
            total = None
            for block in range(GROUP):
                shift = ((block - i) * loads) % LANES
                moved = pltpu.roll(lines[block], shift, 1) if shift else lines[block]
                total = moved if total is None else jnp.where(lane_piece < block * loads, total, moved)
            packed[f, i * piece : (i + 1) * piece, :] = total

    def give(index, carry):
        peer, where = peer_of(me, index, devices, col_count)
        pack_piece(peer)
        pltpu.make_async_remote_copy(
            src_ref=packed.at[peer],
            dst_ref=arrived.at[me],
            send_sem=back_send_sem,
            recv_sem=back_recv_sem,
            device_id=where,
            device_id_type=MESH,
        ).start()
        return carry

    lax.fori_loop(1, devices, give, 0)
    pack_piece(me)
    own = pltpu.make_async_copy(packed.at[me], arrived.at[me], own_sem)
    own.start()
    own.wait()
    out_copy.wait()
    _, where = peer_of(me, 1, devices, col_count)
    every = pltpu.make_async_remote_copy(
        src_ref=packed.at[pl.ds(0, devices - 1)],
        dst_ref=arrived.at[pl.ds(0, devices - 1)],
        send_sem=back_send_sem,
        recv_sem=back_recv_sem,
        device_id=where,
        device_id_type=MESH,
    )
    every.wait_send()
    every.wait_recv()


def main(slots, places, residual, restriction, present, inverse, blocks, pattern, row_count, col_count):
    loads = residual.shape[0]
    residual = residual.transpose(1, 0, 2)
    devices = row_count * col_count
    parts = LANES // devices
    width = LANES * GROUP * PAIR
    pairs = AGG_DEV // width
    present = present.reshape(-1, GROUP * PAIR, LANES)
    height = inverse.shape[2]
    rows = 3 * PAIR * parts
    piece = pairs * PAIR * parts
    planes = 3 * loads
    steps = ITERS - 1
    span = max(planes // HALVES, height)
    cells = height * LANES
    dma = pltpu.SemaphoreType.DMA
    scratch = [pltpu.SMEM((cells // SLOT_REFS,), jnp.int32) for _ in range(SLOT_REFS)] + [
        pltpu.SMEM((cells,), jnp.int32),
        pltpu.VMEM((pairs, FPA, 3, loads, width), jnp.float32),
        pltpu.VMEM((pairs, FPA, 3, 3, width), jnp.float32),
        pltpu.VMEM(present.shape, jnp.int32),
        pltpu.VMEM(inverse.shape, jnp.float32),
        pltpu.VMEM(blocks.shape, jnp.float32),
        pltpu.VMEM(pattern.shape, jnp.int32),
        pltpu.VMEM((3, LANES, LANES), jnp.float32),
        pltpu.VMEM((pairs, devices, rows, LANES), jnp.float32),
        pltpu.VMEM((pairs, devices, rows, LANES), jnp.float32),
        pltpu.VMEM((AGG_DEV, LANES), jnp.float32),
        pltpu.VMEM((cells, LANES), jnp.float32),
        pltpu.VMEM((planes * height, LANES), jnp.float32),
        pltpu.VMEM((planes * height, LANES), jnp.float32),
        pltpu.VMEM((planes, height, LANES), jnp.float32),
        pltpu.VMEM((2, planes, height + 16, LANES), jnp.float32),
        pltpu.VMEM((4, 3, 3, height, LANES), jnp.float32),
        pltpu.VMEM((steps, HALVES, 4, span, LANES), jnp.float32),
        pltpu.VMEM((steps, HALVES, 4, span, LANES), jnp.float32),
        pltpu.VMEM((devices, 3 * piece, LANES), jnp.float32),
        dma((pairs,)),
        dma((pairs,)),
        dma((5,)),
        dma((SLOT_REFS,)),
        dma,
        dma,
        dma((steps, HALVES, 4)),
        dma((steps, HALVES, 4)),
        dma,
        dma,
        dma,
    ]
    return pl.pallas_call(
        functools.partial(main_kernel, row_count, col_count, loads),
        in_specs=[spec_any()] * 8,
        out_specs=(spec_any(), spec_any()),
        out_shape=(
            jax.ShapeDtypeStruct((devices, 3 * piece, LANES), jnp.float32),
            jax.ShapeDtypeStruct((planes * height, LANES), jnp.float32),
        ),
        scratch_shapes=scratch,
        compiler_params=pltpu.CompilerParams(vmem_limit_bytes=VMEM_LIMIT, collective_id=1, has_side_effects=True),
        name="correct",
    )(slots, places, residual, restriction, present, inverse, blocks, pattern)


def prolong_kernel(devices, loads, chunk_ref, restriction_ref, pattern_ref, planes_ref, out_ref, iterate_ref, values):
    groups = AGG_DEV // (LANES * GROUP)
    parts = LANES // devices
    rows = 3 * groups * parts

    @pl.when(pl.program_id(0) == 0)
    def _():
        for i in range(3):
            for group in range(groups):
                start = i * groups * parts + group * parts
                pieces = [chunk_ref[pl.ds(start + part, devices, stride=rows), :] for part in range(parts)]
                values[i, group] = jnp.concatenate(pieces, axis=0).T if parts > 1 else pieces[0].T

    for q in range(planes_ref.shape[1]):
        for i in range(3):
            iterate_ref[q, i] = planes_ref[i, q]

    for group in range(groups):
        for block in range(GROUP):
            b = group * GROUP + block
            lanes = slice(b * LANES, (b + 1) * LANES)
            present = pattern_ref[b : b + 1, :].astype(jnp.float32)
            terms = [values[i, group, block * loads : (block + 1) * loads, :] * present for i in range(3)]
            for j in range(3):
                total = restriction_ref[0, j : j + 1, lanes] * terms[0]
                total = total + restriction_ref[1, j : j + 1, lanes] * terms[1]
                out_ref[j, :, lanes] = total + restriction_ref[2, j : j + 1, lanes] * terms[2]


def prolong(chunks, restriction, pattern, planes, devices, loads, height):
    pattern = pattern.reshape(-1, LANES)
    blocks = AGG_DEV // LANES
    groups = blocks // GROUP
    some = loads // FPA
    out, iterate = pl.pallas_call(
        functools.partial(prolong_kernel, devices, loads),
        grid=(FPA,),
        in_specs=[
            pl.BlockSpec(chunks.shape, lambda p: (0, 0)),
            pl.BlockSpec((3, 3, AGG_DEV), lambda p: (0, 0, p)),
            pl.BlockSpec((blocks, LANES), lambda p: (p, 0)),
            pl.BlockSpec((3, some, height, LANES), lambda p: (0, p, 0, 0)),
        ],
        out_specs=(
            pl.BlockSpec((3, loads, AGG_DEV), lambda p: (0, 0, p)),
            pl.BlockSpec((some, 3, height, LANES), lambda p: (p, 0, 0, 0)),
        ),
        out_shape=(
            jax.ShapeDtypeStruct((3, loads, restriction.shape[2]), jnp.float32),
            jax.ShapeDtypeStruct((loads, 3, height, LANES), jnp.float32),
        ),
        scratch_shapes=[pltpu.VMEM((3, groups, GROUP * loads, LANES), jnp.float32)],
        compiler_params=pltpu.CompilerParams(vmem_limit_bytes=VMEM_LIMIT),
        name="prolong",
    )(chunks, restriction, pattern, planes.reshape(3, loads, height, LANES))
    return out.transpose(1, 0, 2), iterate


def body(
    fine_residual,
    restriction,
    restriction_pattern,
    cell_aggregate,
    block_inverse,
    off_blocks,
    operator_pattern,
):
    loads = fine_residual.shape[0]
    row_count = lax.axis_size("row")
    col_count = lax.axis_size("col")
    devices = row_count * col_count
    height = cell_aggregate.shape[0]
    slots, places = tables(cell_aggregate, devices)
    arrived, planes = main(
        slots,
        places,
        fine_residual,
        restriction,
        restriction_pattern,
        block_inverse,
        off_blocks,
        operator_pattern,
        row_count,
        col_count,
    )
    fine_correction, iterate = prolong(
        arrived.reshape(-1, LANES), restriction, restriction_pattern, planes, devices, loads, height
    )
    return (iterate, fine_correction)


def solution(mesh):
    in_specs = (
        P(None, None, ("row", "col")),
        P(None, None, ("row", "col")),
        P(("row", "col")),
        P("row", "col"),
        P(None, None, "row", "col"),
        P(None, None, None, "row", "col"),
        P(None, "row", "col"),
    )
    out_specs = (P(None, None, "row", "col"), P(None, None, ("row", "col")))
    return jax.shard_map(body, mesh=mesh, in_specs=in_specs, out_specs=out_specs, check_vma=False)
```

```python
import functools

import jax
import jax.numpy as jnp
from jax import lax
from jax.experimental import pallas as pl
from jax.experimental.pallas import tpu as pltpu
from jax.sharding import PartitionSpec as P

FPA = 8
ITERS = 4
AGG_DEV = 6144
LANES = 128
GROUP = 8
PAIR = 2
HALVES = 2
SLOT_REFS = 6
MESH = pl.DeviceIdType.MESH
VMEM_LIMIT = 56 * 1024 * 1024


def spec_vmem():
    return pl.BlockSpec(memory_space=pltpu.VMEM)


def spec_any():
    return pl.BlockSpec(memory_space=pl.ANY)


def peer_of(me, index, devices, col_count):
    peer = lax.rem(me + index, devices)
    return peer, {"row": peer // col_count, "col": lax.rem(peer, col_count)}


def greet(devices, col_count, me):
    barrier = pltpu.get_barrier_semaphore()

    def signal(index, carry):
        _, where = peer_of(me, index, devices, col_count)
        pl.semaphore_signal(barrier, inc=1, device_id=where, device_id_type=MESH)
        return carry

    lax.fori_loop(1, devices, signal, 0)
    return barrier


def fill_tables(devices, cells_ref, slots_ref, inverse_ref, total_ref, owner_ref):
    height = cells_ref.shape[0]
    parts = LANES // devices
    blocks = AGG_DEV // LANES
    piece = blocks * parts // GROUP
    value = cells_ref[...].astype(jnp.float32)
    owner = jnp.floor((value + 0.5) * (1.0 / AGG_DEV))
    inside = value - owner * AGG_DEV
    block = jnp.floor((inside + 0.5) * (1.0 / LANES))
    part = jnp.floor((inside - block * LANES + 0.5) * (1.0 / devices))
    group = jnp.floor((block + 0.5) * (1.0 / GROUP))
    slot = owner * (GROUP * piece) + (block - group * GROUP) * piece + group * parts + part
    slots_ref[...] = jnp.clip(slot.astype(jnp.int32), 0, AGG_DEV - 1)
    owner_ref[0] = block
    owner_ref[1] = part * devices + owner
    rows = lax.broadcasted_iota(jnp.int32, (blocks, LANES), 0).astype(jnp.float32)
    lanes = lax.broadcasted_iota(jnp.int32, (blocks, LANES), 1).astype(jnp.float32)
    places = lax.broadcasted_iota(jnp.int32, (LANES, LANES), 0).astype(jnp.float32)
    total_ref[...] = jnp.zeros_like(total_ref)

    def some(r, carry):
        hit = rows == owner_ref[0, pl.ds(r, 1), :]
        low = jnp.where(hit, lanes, 0.0)
        high = jnp.where(hit, r.astype(jnp.float32), 0.0)
        left = jnp.concatenate([low, high], axis=0).astype(jnp.bfloat16)
        right = jnp.where(places == owner_ref[1, pl.ds(r, 1), :], 1.0, 0.0).astype(jnp.bfloat16)
        total_ref[...] += lax.dot_general(left, right, (((1,), (1,)), ((), ())), preferred_element_type=jnp.float32)
        return carry

    lax.fori_loop(0, height, some, 0, unroll=4)
    inverse = (total_ref[:blocks] + total_ref[blocks:] * LANES).astype(jnp.int32)
    inverse_ref[...] = jnp.clip(inverse, 0, height * LANES - 1)


def main_kernel(row_count, col_count, loads, *refs):
    (
        cells_hbm,
        residual_hbm,
        restriction_hbm,
        present_hbm,
        inverse_hbm,
        blocks_hbm,
        pattern_hbm,
        values_hbm,
        planes_hbm,
    ) = refs[:9]
    slots = refs[9 : 9 + SLOT_REFS]
    (
        places,
        cells,
        slots_all,
        places_all,
        total,
        digits,
        residual,
        restriction,
        present_all,
        inverse_ref,
        blocks_ref,
        pattern_ref,
        stage,
        sent,
        chunk,
        table,
        ordered,
        rhs,
        planes_ref,
        base,
        x,
        mixed,
        edge,
        halo,
        packed,
        arrived,
        values,
        residual_sem,
        small_sem,
        slots_sem,
        send_sem,
        recv_sem,
        halo_send_sem,
        halo_recv_sem,
        back_send_sem,
        back_recv_sem,
        values_sem,
    ) = refs[9 + SLOT_REFS :]
    devices = row_count * col_count
    parts = LANES // devices
    pairs = residual.shape[0]
    width = residual.shape[-1]
    height = inverse_ref.shape[2]
    few = PAIR * parts
    piece = pairs * few
    row = lax.axis_index("row")
    col = lax.axis_index("col")
    me = row * col_count + col
    rows = 3 * few
    small = [
        pltpu.make_async_copy(present_hbm, present_all, small_sem.at[0]),
        pltpu.make_async_copy(restriction_hbm, restriction, small_sem.at[1]),
        pltpu.make_async_copy(cells_hbm, cells, small_sem.at[2]),
        pltpu.make_async_copy(inverse_hbm, inverse_ref, small_sem.at[3]),
        pltpu.make_async_copy(blocks_hbm, blocks_ref, small_sem.at[4]),
        pltpu.make_async_copy(pattern_hbm, pattern_ref, small_sem.at[5]),
    ]

    def load(pair):
        for p in range(FPA):
            lanes = pl.ds((p * pairs + pair) * width, width)
            pltpu.make_async_copy(residual_hbm.at[:, :, lanes], residual.at[pair, p], residual_sem.at[pair]).start()

    small[0].start()
    load(0)
    small[1].start()
    barrier = greet(devices, col_count, me)
    for pair in range(1, pairs):
        load(pair)
    for copy in small[2:]:
        copy.start()
    halo[...] = jnp.zeros_like(halo)
    small[0].wait()
    small[1].wait()

    def send_first(pair):
        def send(index, carry):
            peer, where = peer_of(me, index, devices, col_count)
            pltpu.make_async_remote_copy(
                src_ref=sent.at[pl.ds((pair * devices + peer) * rows, rows)],
                dst_ref=chunk.at[pair, me],
                send_sem=send_sem,
                recv_sem=recv_sem,
                device_id=where,
                device_id_type=MESH,
            ).start()
            return carry

        lax.fori_loop(1, devices, send, 0)

    def restrict(pair):
        pltpu.make_async_copy(residual.at[pair], residual.at[pair], residual_sem.at[pair]).wait()
        for half in range(PAIR):
            for block in range(GROUP):
                start = (half * GROUP + block) * LANES
                lanes = slice(start, start + LANES)
                which = half * GROUP + block
                totals = [None, None, None]
                for p in range(FPA):
                    there = pl.ds(pl.multiple_of((p * pairs + pair) * width + start, LANES), LANES)
                    present = present_all[p * pairs + pair, which : which + 1, :].astype(jnp.float32)
                    for j in range(3):
                        masked = residual[pair, p, j, :, lanes] * present
                        for i in range(3):
                            term = restriction[i, j : j + 1, there] * masked
                            totals[i] = term if totals[i] is None else totals[i] + term
                for i in range(3):
                    stage[i, block * loads : (block + 1) * loads, :] = totals[i]
            for i in range(3):
                turned = stage[i].T
                for part in range(parts):
                    at = pair * (devices * rows) + (i * PAIR + half) * parts + part
                    sent[pl.ds(at, devices, stride=rows), :] = turned[part * devices : (part + 1) * devices, :]

    restrict(0)
    pl.semaphore_wait(barrier, devices - 1)
    send_first(0)

    def later(pair, carry):
        restrict(pair)
        send_first(pair)
        return carry

    lax.fori_loop(1, pairs, later, 0)
    for copy in small[2:]:
        copy.wait()

    def keep(pair, carry):
        chunk[pair, me] = sent[pl.ds((pair * devices + me) * rows, rows), :]
        return carry

    lax.fori_loop(0, pairs, keep, 0)

    def fold(d, carry):
        on = pattern_ref[d].astype(jnp.float32)
        for k in range(3):
            column = [blocks_ref[d, j, k] * on for j in range(3)]
            for i in range(3):
                total = inverse_ref[i, 0] * column[0]
                total = total + inverse_ref[i, 1] * column[1]
                mixed[d, i, k] = total + inverse_ref[i, 2] * column[2]
        return carry

    lax.fori_loop(0, 4, fold, 0)
    fill_tables(devices, cells, slots_all, places_all, total, digits)
    lines = slots[0].shape[0]
    span = lines * LANES
    moves = [pltpu.make_async_copy(places_all, places, small_sem.at[0])]
    for n in range(SLOT_REFS):
        moves.append(pltpu.make_async_copy(slots_all.at[pl.ds(n * lines, lines)], slots[n], slots_sem.at[n]))
    for move in moves:
        move.start()
    for move in moves:
        move.wait()
    _, where = peer_of(me, 1, devices, col_count)
    every = pltpu.make_async_remote_copy(
        src_ref=chunk.at[:, pl.ds(0, devices - 1)],
        dst_ref=chunk.at[:, pl.ds(0, devices - 1)],
        send_sem=send_sem,
        recv_sem=recv_sem,
        device_id=where,
        device_id_type=MESH,
    )
    every.wait_send()
    every.wait_recv()

    lane_few = lax.broadcasted_iota(jnp.int32, (few, LANES), 1) // loads

    def unpack(f, carry):
        for pair in range(pairs):
            parts_i = [chunk[pair, f, i * few : (i + 1) * few, :] for i in range(3)]
            moved = [parts_i[0], pltpu.roll(parts_i[1], loads, 1), pltpu.roll(parts_i[2], 2 * loads, 1)]
            for group in ((0, 3), (1, 4), (2, 5), (6,), (7,)):
                second = functools.reduce(jnp.logical_or, [lane_few == (b + 1) % GROUP for b in group])
                third = functools.reduce(jnp.logical_or, [lane_few == (b + 2) % GROUP for b in group])
                mix = jnp.where(third, moved[2], jnp.where(second, moved[1], moved[0]))
                for b in group:
                    line = pltpu.roll(mix, (LANES - b * loads) % LANES, 1) if b else mix
                    table[pl.ds(f * (GROUP * piece) + b * piece + pair * few, few), :] = line
        return carry

    lax.fori_loop(0, devices, unpack, 0, unroll=4)

    def take(line, carry):
        for j in range(LANES):
            for n in range(SLOT_REFS):
                ordered[pl.ds(n * span + line * LANES + j, 1), :] = table[pl.ds(slots[n][line, j], 1), :]
        return carry

    lax.fori_loop(0, lines, take, 0)

    def turn(r, carry):
        turned = ordered[pl.ds(pl.multiple_of(r * LANES, LANES), LANES), :].T
        rhs[pl.ds(r, 3 * loads, stride=height), :] = turned[: 3 * loads, :]
        return carry

    lax.fori_loop(0, height, turn, 0, unroll=12)

    part_loads = loads // HALVES
    planes = 3 * part_loads
    exists = (row > 0, row < row_count - 1, col > 0, col < col_count - 1)
    peers = (
        {"row": row - 1, "col": col},
        {"row": row + 1, "col": col},
        {"row": row, "col": col - 1},
        {"row": row, "col": col + 1},
    )
    extent = (planes, planes, height, height)
    lane = lax.broadcasted_iota(jnp.int32, (height, LANES), 1)

    def plane_rows(index):
        return pl.ds(pl.multiple_of(index * height, height), height)

    def first(half):
        def one(q, carry):
            source = half * part_loads + q
            given = [rhs[plane_rows(j * loads + source), :] for j in range(3)]
            for i in range(3):
                total = inverse_ref[i, 0] * given[0]
                total = total + inverse_ref[i, 1] * given[1]
                total = total + inverse_ref[i, 2] * given[2]
                base[half * planes + i * part_loads + q] = total
                x[0, half * planes + i * part_loads + q, 8 : 8 + height, :] = total
            return carry

        lax.fori_loop(0, part_loads, one, 0, unroll=2)

    def pack(slot, step, half):
        own = slice(half * planes, (half + 1) * planes)
        edge[step, half, 0, :planes, :] = x[slot, own, 8, :]
        edge[step, half, 1, :planes, :] = x[slot, own, 7 + height, :]

        def columns(p, carry):
            left, right = carry
            plane = x[slot, half * planes + p, 8 : 8 + height, :]
            left = jnp.where(lane == p, pltpu.roll(plane, p, 1), left)
            right = jnp.where(lane == p, pltpu.roll(plane, p + 1, 1), right)
            return left, right

        blank = jnp.zeros((height, LANES), jnp.float32)
        left, right = lax.fori_loop(0, planes, columns, (blank, blank), unroll=12)
        edge[step, half, 2, :height, :] = left
        edge[step, half, 3, :height, :] = right

    def copy_edge(step, half, d, side):
        return pltpu.make_async_remote_copy(
            src_ref=edge.at[step, half, d, pl.ds(0, extent[d])],
            dst_ref=halo.at[step, half, side, pl.ds(0, extent[d])],
            send_sem=halo_send_sem.at[step, half, d],
            recv_sem=halo_recv_sem.at[step, half, side],
            device_id=peers[d],
            device_id_type=MESH,
        )

    def start(step, half):
        for d in range(4):

            @pl.when(exists[d])
            def _():
                copy_edge(step, half, d, d ^ 1).start()

    for half in range(HALVES):
        first(half)
        pack(0, 0, half)
        start(0, half)
    for step in range(ITERS - 1):
        old = step % 2
        last = step == ITERS - 2
        for half in range(HALVES):
            for d in range(4):

                @pl.when(exists[d])
                def _():
                    copy_edge(step, half, d, d).wait_send()
                    copy_edge(step, half, d, d).wait_recv()

            own = slice(half * planes, (half + 1) * planes)
            x[old, own, 7, :] = halo[step, half, 0, :planes, :]
            x[old, own, 8 + height, :] = halo[step, half, 1, :planes, :]

            def update(q, carry):
                totals = [base[half * planes + i * part_loads + q] for i in range(3)]
                for k in range(3):
                    local = k * part_loads + q
                    p = half * planes + local
                    plane = x[old, p, 8 : 8 + height, :]
                    left = jnp.where(
                        lane == 0,
                        pltpu.roll(halo[step, half, 2, :height, :], lax.rem(LANES - local, LANES), 1),
                        pltpu.roll(plane, 1, 1),
                    )
                    right = jnp.where(
                        lane == LANES - 1,
                        pltpu.roll(halo[step, half, 3, :height, :], LANES - 1 - local, 1),
                        pltpu.roll(plane, LANES - 1, 1),
                    )
                    shifted = (x[old, p, 7 : 7 + height, :], x[old, p, 9 : 9 + height, :], left, right)
                    for d in range(4):
                        for i in range(3):
                            totals[i] = totals[i] - mixed[d, i, k] * shifted[d]
                for i in range(3):
                    if last:
                        planes_ref[plane_rows(i * loads + half * part_loads + q), :] = totals[i]
                    else:
                        x[1 - old, half * planes + i * part_loads + q, 8 : 8 + height, :] = totals[i]
                return carry

            lax.fori_loop(0, part_loads, update, 0, unroll=2)
            if not last:
                pack(1 - old, step + 1, half)
                start(step + 1, half)

    out_copy = pltpu.make_async_copy(planes_ref, planes_hbm, small_sem.at[0])
    out_copy.start()

    def back(r, carry):
        plane = planes_ref[pl.ds(r, 3 * loads, stride=height), :]
        ordered[pl.ds(pl.multiple_of(r * LANES, LANES), LANES), : 3 * loads] = plane.T
        return carry

    lax.fori_loop(0, height, back, 0, unroll=12)
    lane_few = lax.broadcasted_iota(jnp.int32, (few, LANES), 1)

    def pack_back(pair, peer, at):
        for block in range(GROUP):
            for n in range(few):
                line = (pair * PAIR + n // parts) * GROUP + block
                source = places[line, (n % parts) * devices + peer]
                table[pl.ds(at + block * few + n, 1), :] = ordered[pl.ds(source, 1), :]
        lines = [table[at + block * few : at + (block + 1) * few, :] for block in range(GROUP)]
        results = []
        for i in range(3):
            result = None
            for block in range(GROUP):
                shift = ((block - i) * loads) % LANES
                moved = pltpu.roll(lines[block], shift, 1) if shift else lines[block]
                result = moved if result is None else jnp.where(lane_few < block * loads, result, moved)
            results.append(result)
        return results

    def place_of(pair, device):
        return (pair * devices + device) * rows

    def give_back(pair, carry):
        def give(step, carry):
            for n in range(2):
                index = 2 * step + 1 + n
                peer, where = peer_of(me, index, devices, col_count)
                results = pack_back(pair, peer, n * GROUP * few)
                for i in range(3):
                    packed[pl.ds(place_of(pair, peer) + i * few, few), :] = results[i]

                def send():
                    pltpu.make_async_remote_copy(
                        src_ref=packed.at[pl.ds(place_of(pair, peer), rows)],
                        dst_ref=arrived.at[pl.ds(place_of(pair, me), rows)],
                        send_sem=back_send_sem.at[pair],
                        recv_sem=back_recv_sem.at[pair],
                        device_id=where,
                        device_id_type=MESH,
                    ).start()

                if n == 0:
                    send()
                else:
                    pl.when(index < devices)(send)
            return carry

        lax.fori_loop(0, devices // 2, give, 0)
        arrived[pl.ds(place_of(pair, me), rows), :] = packed[pl.ds(place_of(pair, me), rows), :]
        return carry

    lax.fori_loop(0, pairs, give_back, 0)
    for pair in range(pairs):
        _, where = peer_of(me, 1, devices, col_count)
        every = pltpu.make_async_remote_copy(
            src_ref=packed.at[pl.ds(place_of(pair, 0), (devices - 1) * rows)],
            dst_ref=arrived.at[pl.ds(place_of(pair, 0), (devices - 1) * rows)],
            send_sem=back_send_sem.at[pair],
            recv_sem=back_recv_sem.at[pair],
            device_id=where,
            device_id_type=MESH,
        )
        every.wait_send()
        every.wait_recv()
        for i in range(3):
            for half in range(PAIR):
                at = place_of(pair, 0) + (i * PAIR + half) * parts
                pieces = [arrived[pl.ds(at + part, devices, stride=rows), :] for part in range(parts)]
                values[pair, i, half] = jnp.concatenate(pieces, axis=0).T if parts > 1 else pieces[0].T
        pltpu.make_async_copy(values.at[pair], values_hbm.at[pair], values_sem.at[pair]).start()
    out_copy.wait()
    for pair in range(pairs):
        pltpu.make_async_copy(values.at[pair], values_hbm.at[pair], values_sem.at[pair]).wait()


def main(cells, residual, restriction, present, inverse, blocks, pattern, row_count, col_count):
    loads = residual.shape[0]
    residual = residual.transpose(1, 0, 2)
    devices = row_count * col_count
    parts = LANES // devices
    width = LANES * GROUP * PAIR
    pairs = AGG_DEV // width
    present = present.reshape(-1, GROUP * PAIR, LANES)
    height = inverse.shape[2]
    rows = 3 * PAIR * parts
    planes = 3 * loads
    steps = ITERS - 1
    span = max(planes // HALVES, height)
    count = height * LANES
    blocks_own = AGG_DEV // LANES
    dma = pltpu.SemaphoreType.DMA
    scratch = [pltpu.SMEM((height // SLOT_REFS, LANES), jnp.int32) for _ in range(SLOT_REFS)] + [
        pltpu.SMEM((blocks_own, LANES), jnp.int32),
        pltpu.VMEM((height, LANES), jnp.int32),
        pltpu.VMEM((height, LANES), jnp.int32),
        pltpu.VMEM((blocks_own, LANES), jnp.int32),
        pltpu.VMEM((2 * blocks_own, LANES), jnp.float32),
        pltpu.VMEM((2, height, LANES), jnp.float32),
        pltpu.VMEM((pairs, FPA, 3, loads, width), jnp.float32),
        pltpu.VMEM(restriction.shape, jnp.float32),
        pltpu.VMEM(present.shape, jnp.int32),
        pltpu.VMEM(inverse.shape, jnp.float32),
        pltpu.VMEM(blocks.shape, jnp.float32),
        pltpu.VMEM(pattern.shape, jnp.int32),
        pltpu.VMEM((3, LANES, LANES), jnp.float32),
        pltpu.VMEM((pairs * devices * rows, LANES), jnp.float32),
        pltpu.VMEM((pairs, devices, rows, LANES), jnp.float32),
        pltpu.VMEM((AGG_DEV, LANES), jnp.float32),
        pltpu.VMEM((count, LANES), jnp.float32),
        pltpu.VMEM((planes * height, LANES), jnp.float32),
        pltpu.VMEM((planes * height, LANES), jnp.float32),
        pltpu.VMEM((planes, height, LANES), jnp.float32),
        pltpu.VMEM((2, planes, height + 16, LANES), jnp.float32),
        pltpu.VMEM((4, 3, 3, height, LANES), jnp.float32),
        pltpu.VMEM((steps, HALVES, 4, span, LANES), jnp.float32),
        pltpu.VMEM((steps, HALVES, 4, span, LANES), jnp.float32),
        pltpu.VMEM((pairs * devices * rows, LANES), jnp.float32),
        pltpu.VMEM((pairs * devices * rows, LANES), jnp.float32),
        pltpu.VMEM((pairs, 3, PAIR, LANES, LANES), jnp.float32),
        dma((pairs,)),
        dma((6,)),
        dma((SLOT_REFS,)),
        dma,
        dma,
        dma((steps, HALVES, 4)),
        dma((steps, HALVES, 4)),
        dma((pairs,)),
        dma((pairs,)),
        dma((pairs,)),
    ]
    return pl.pallas_call(
        functools.partial(main_kernel, row_count, col_count, loads),
        in_specs=[spec_any()] * 7,
        out_specs=(spec_any(), spec_any()),
        out_shape=(
            jax.ShapeDtypeStruct((pairs, 3, PAIR, LANES, LANES), jnp.float32),
            jax.ShapeDtypeStruct((planes * height, LANES), jnp.float32),
        ),
        scratch_shapes=scratch,
        compiler_params=pltpu.CompilerParams(vmem_limit_bytes=VMEM_LIMIT, collective_id=1, has_side_effects=True),
        name="correct",
    )(cells, residual, restriction, present, inverse, blocks, pattern)


def prolong_kernel(
    values_hbm,
    restriction_hbm,
    pattern_hbm,
    planes_hbm,
    out_hbm,
    iterate_hbm,
    values,
    restriction,
    pattern,
    planes,
    out,
    restriction_sem,
    small_sem,
    out_sem,
    iterate_sem,
):
    pairs = values.shape[0]
    loads = out.shape[1]
    blocks = AGG_DEV // LANES

    def slab(p):
        return pl.ds(pl.multiple_of(p * AGG_DEV, LANES), AGG_DEV)

    def restriction_copy(p):
        return pltpu.make_async_copy(restriction_hbm.at[:, :, slab(p)], restriction.at[:, :, slab(p)], restriction_sem.at[p])

    def out_copy(p):
        return pltpu.make_async_copy(out.at[:, :, slab(p)], out_hbm.at[:, :, slab(p)], out_sem.at[p])

    small = [
        pltpu.make_async_copy(pattern_hbm, pattern, small_sem.at[0]),
        pltpu.make_async_copy(values_hbm, values, small_sem.at[1]),
        pltpu.make_async_copy(planes_hbm, planes, small_sem.at[2]),
    ]
    small[1].start()
    restriction_copy(0).start()
    small[0].start()
    for p in range(1, FPA):
        restriction_copy(p).start()
    small[2].start()
    small[0].wait()
    small[1].wait()

    def one(p, carry):
        restriction_copy(p).wait()
        for b in range(blocks):
            pair, half, block = b // (GROUP * PAIR), b // GROUP % PAIR, b % GROUP
            lanes = pl.ds(pl.multiple_of(p * AGG_DEV + b * LANES, LANES), LANES)
            present = pattern[pl.ds(p * blocks + b, 1), :].astype(jnp.float32)
            terms = [values[pair, i, half, block * loads : (block + 1) * loads, :] * present for i in range(3)]
            for j in range(3):
                total = restriction[0, j : j + 1, lanes] * terms[0]
                total = total + restriction[1, j : j + 1, lanes] * terms[1]
                out[j, :, lanes] = total + restriction[2, j : j + 1, lanes] * terms[2]
        out_copy(p).start()
        return carry

    lax.fori_loop(0, FPA, one, 0)
    small[2].wait()
    turned = [pltpu.make_async_copy(planes.at[i], iterate_hbm.at[:, i], iterate_sem.at[i]) for i in range(3)]
    for copy in turned:
        copy.start()
    for copy in turned:
        copy.wait()
    for p in range(FPA):
        out_copy(p).wait()


def prolong(values, restriction, pattern, planes, loads, height):
    pattern = pattern.reshape(-1, LANES)
    planes = planes.reshape(3, loads, height, LANES)
    dma = pltpu.SemaphoreType.DMA
    shape = (3, loads, restriction.shape[2])
    out, iterate = pl.pallas_call(
        prolong_kernel,
        in_specs=[spec_any()] * 4,
        out_specs=(spec_any(), spec_any()),
        out_shape=(
            jax.ShapeDtypeStruct(shape, jnp.float32),
            jax.ShapeDtypeStruct((loads, 3, height, LANES), jnp.float32),
        ),
        scratch_shapes=[
            pltpu.VMEM(values.shape, jnp.float32),
            pltpu.VMEM(restriction.shape, jnp.float32),
            pltpu.VMEM(pattern.shape, jnp.int32),
            pltpu.VMEM(planes.shape, jnp.float32),
            pltpu.VMEM(shape, jnp.float32),
            dma((FPA,)),
            dma((3,)),
            dma((FPA,)),
            dma((3,)),
        ],
        compiler_params=pltpu.CompilerParams(vmem_limit_bytes=VMEM_LIMIT),
        name="prolong",
    )(values, restriction, pattern, planes)
    return out.transpose(1, 0, 2), iterate


def body(
    fine_residual,
    restriction,
    restriction_pattern,
    cell_aggregate,
    block_inverse,
    off_blocks,
    operator_pattern,
):
    loads = fine_residual.shape[0]
    row_count = lax.axis_size("row")
    col_count = lax.axis_size("col")
    height = cell_aggregate.shape[0]
    values, planes = main(
        cell_aggregate,
        fine_residual,
        restriction,
        restriction_pattern,
        block_inverse,
        off_blocks,
        operator_pattern,
        row_count,
        col_count,
    )
    fine_correction, iterate = prolong(values, restriction, restriction_pattern, planes, loads, height)
    return (iterate, fine_correction)


def solution(mesh):
    in_specs = (
        P(None, None, ("row", "col")),
        P(None, None, ("row", "col")),
        P(("row", "col")),
        P("row", "col"),
        P(None, None, "row", "col"),
        P(None, None, None, "row", "col"),
        P(None, "row", "col"),
    )
    out_specs = (P(None, None, "row", "col"), P(None, None, ("row", "col")))
    return jax.shard_map(body, mesh=mesh, in_specs=in_specs, out_specs=out_specs, check_vma=False)
```

```python
import functools

import jax
import jax.numpy as jnp
from jax import lax
from jax.experimental import pallas as pl
from jax.experimental.pallas import tpu as pltpu
from jax.sharding import PartitionSpec as P

FPA = 8
ITERS = 4
AGG_DEV = 6144
LANES = 128
GROUP = 8
PAIR = 2
HALVES = 4
BATCH = 8
SLOT_REFS = 6
MESH = pl.DeviceIdType.MESH
VMEM_LIMIT = 56 * 1024 * 1024


def spec_vmem():
    return pl.BlockSpec(memory_space=pltpu.VMEM)


def spec_any():
    return pl.BlockSpec(memory_space=pl.ANY)


def peer_of(me, index, devices, col_count):
    peer = lax.rem(me + index, devices)
    return peer, {"row": peer // col_count, "col": lax.rem(peer, col_count)}


def greet(devices, col_count, me):
    barrier = pltpu.get_barrier_semaphore()

    def signal(index, carry):
        _, where = peer_of(me, index, devices, col_count)
        pl.semaphore_signal(barrier, inc=1, device_id=where, device_id_type=MESH)
        return carry

    lax.fori_loop(1, devices, signal, 0)
    return barrier


def fill_tables(devices, cells_ref, slots_ref, inverse_ref, total_ref, owner_ref):
    height = cells_ref.shape[0]
    parts = LANES // devices
    blocks = AGG_DEV // LANES
    piece = blocks * parts // GROUP
    value = cells_ref[...].astype(jnp.float32)
    owner = jnp.floor((value + 0.5) * (1.0 / AGG_DEV))
    inside = value - owner * AGG_DEV
    block = jnp.floor((inside + 0.5) * (1.0 / LANES))
    part = jnp.floor((inside - block * LANES + 0.5) * (1.0 / devices))
    group = jnp.floor((block + 0.5) * (1.0 / GROUP))
    slot = owner * (GROUP * piece) + (block - group * GROUP) * piece + group * parts + part
    slots_ref[...] = jnp.clip(slot.astype(jnp.int32), 0, AGG_DEV - 1)
    owner_ref[0] = block
    owner_ref[1] = part * devices + owner
    rows = lax.broadcasted_iota(jnp.int32, (blocks, LANES), 0).astype(jnp.float32)
    lanes = lax.broadcasted_iota(jnp.int32, (blocks, LANES), 1).astype(jnp.float32)
    places = lax.broadcasted_iota(jnp.int32, (LANES, LANES), 0).astype(jnp.float32)
    total_ref[...] = jnp.zeros_like(total_ref)

    def some(r, carry):
        hit = rows == owner_ref[0, pl.ds(r, 1), :]
        low = jnp.where(hit, lanes, 0.0)
        high = jnp.where(hit, r.astype(jnp.float32), 0.0)
        left = jnp.concatenate([low, high], axis=0).astype(jnp.bfloat16)
        right = jnp.where(places == owner_ref[1, pl.ds(r, 1), :], 1.0, 0.0).astype(jnp.bfloat16)
        total_ref[...] += lax.dot_general(left, right, (((1,), (1,)), ((), ())), preferred_element_type=jnp.float32)
        return carry

    lax.fori_loop(0, height, some, 0, unroll=4)
    inverse = (total_ref[:blocks] + total_ref[blocks:] * LANES).astype(jnp.int32)
    inverse_ref[...] = jnp.clip(inverse, 0, height * LANES - 1)


def main_kernel(row_count, col_count, loads, *refs):
    (
        cells_hbm,
        residual_hbm,
        restriction_hbm,
        present_hbm,
        inverse_hbm,
        blocks_hbm,
        pattern_hbm,
        values_hbm,
        planes_hbm,
    ) = refs[:9]
    slots = refs[9 : 9 + SLOT_REFS]
    (
        places,
        cells,
        slots_all,
        places_all,
        total,
        digits,
        residual,
        restriction,
        present_all,
        inverse_ref,
        blocks_ref,
        pattern_ref,
        stage,
        sent,
        chunk,
        table,
        ordered,
        rhs,
        planes_ref,
        base,
        x,
        mixed,
        edge,
        halo,
        both,
        packed,
        arrived,
        values,
        residual_sem,
        restriction_sem,
        small_sem,
        slots_sem,
        send_sem,
        recv_sem,
        halo_send_sem,
        halo_recv_sem,
        back_send_sem,
        back_recv_sem,
        values_sem,
    ) = refs[9 + SLOT_REFS :]
    devices = row_count * col_count
    parts = LANES // devices
    pairs = residual.shape[0]
    width = residual.shape[-1]
    height = inverse_ref.shape[2]
    few = PAIR * parts
    piece = pairs * few
    row = lax.axis_index("row")
    col = lax.axis_index("col")
    me = row * col_count + col
    rows = 3 * few
    half_width = width // PAIR
    small = [
        pltpu.make_async_copy(present_hbm, present_all, small_sem.at[0]),
        pltpu.make_async_copy(cells_hbm, cells, small_sem.at[1]),
        pltpu.make_async_copy(inverse_hbm, inverse_ref, small_sem.at[2]),
        pltpu.make_async_copy(blocks_hbm, blocks_ref, small_sem.at[3]),
        pltpu.make_async_copy(pattern_hbm, pattern_ref, small_sem.at[4]),
    ]

    def load(pair, first_lane, count, which):
        for p in range(FPA):
            lanes = pl.ds((p * pairs + pair) * width + first_lane, count)
            target = residual.at[pair, p, :, :, pl.ds(first_lane, count)]
            pltpu.make_async_copy(residual_hbm.at[:, :, lanes], target, residual_sem.at[which]).start()
            target = restriction.at[:, :, lanes]
            pltpu.make_async_copy(restriction_hbm.at[:, :, lanes], target, restriction_sem.at[which]).start()

    def loaded(pair, first_lane, count, which):
        target = residual.at[pair, :, :, :, pl.ds(first_lane, count)]
        pltpu.make_async_copy(target, target, residual_sem.at[which]).wait()
        target = restriction.at[:, :, pl.ds(0, FPA * count)]
        pltpu.make_async_copy(target, target, restriction_sem.at[which]).wait()

    small[0].start()
    load(0, 0, half_width, 0)
    load(0, half_width, half_width, pairs)
    barrier = greet(devices, col_count, me)
    for pair in range(1, pairs):
        load(pair, 0, width, pair)
    for copy in small[1:]:
        copy.start()
    halo[...] = jnp.zeros_like(halo)
    small[0].wait()

    near = devices // 2

    def send_first(pair):
        def send(index, carry):
            peer, where = peer_of(me, index, devices, col_count)
            pltpu.make_async_remote_copy(
                src_ref=sent.at[pl.ds((pair * devices + peer) * rows, rows)],
                dst_ref=chunk.at[pair, me],
                send_sem=send_sem,
                recv_sem=recv_sem.at[pair, index // near],
                device_id=where,
                device_id_type=MESH,
            ).start()
            return carry

        lax.fori_loop(1, devices, send, 0)

    def restrict(pair, split):
        if not split:
            loaded(pair, 0, width, pair)
        for half in range(PAIR):
            if split:
                loaded(pair, half * half_width, half_width, pairs if half else 0)
            for block in range(GROUP):
                start = (half * GROUP + block) * LANES
                lanes = slice(start, start + LANES)
                which = half * GROUP + block
                totals = [None, None, None]
                for p in range(FPA):
                    there = pl.ds(pl.multiple_of((p * pairs + pair) * width + start, LANES), LANES)
                    present = present_all[p * pairs + pair, which : which + 1, :].astype(jnp.float32)
                    for j in range(3):
                        masked = residual[pair, p, j, :, lanes] * present
                        for i in range(3):
                            term = restriction[i, j : j + 1, there] * masked
                            totals[i] = term if totals[i] is None else totals[i] + term
                for i in range(3):
                    stage[i, block * loads : (block + 1) * loads, :] = totals[i]
            for i in range(3):
                turned = stage[i].T
                for part in range(parts):
                    at = pair * (devices * rows) + (i * PAIR + half) * parts + part
                    sent[pl.ds(at, devices, stride=rows), :] = turned[part * devices : (part + 1) * devices, :]

    restrict(0, True)
    pl.semaphore_wait(barrier, devices - 1)
    send_first(0)

    def later(pair, carry):
        restrict(pair, False)
        send_first(pair)
        return carry

    lax.fori_loop(1, pairs, later, 0)
    for copy in small[1:]:
        copy.wait()

    def keep(pair, carry):
        chunk[pair, me] = sent[pl.ds((pair * devices + me) * rows, rows), :]
        return carry

    lax.fori_loop(0, pairs, keep, 0)

    def fold(d, carry):
        on = pattern_ref[d].astype(jnp.float32)
        for k in range(3):
            column = [blocks_ref[d, j, k] * on for j in range(3)]
            for i in range(3):
                total = inverse_ref[i, 0] * column[0]
                total = total + inverse_ref[i, 1] * column[1]
                mixed[d, i, k] = total + inverse_ref[i, 2] * column[2]
        return carry

    lax.fori_loop(0, 4, fold, 0)
    fill_tables(devices, cells, slots_all, places_all, total, digits)
    lines = slots[0].shape[0]
    moves = [pltpu.make_async_copy(places_all, places, small_sem.at[0])]
    for n in range(SLOT_REFS):
        moves.append(pltpu.make_async_copy(slots_all.at[pl.ds(n * lines, lines)], slots[n], slots_sem.at[n]))
    for move in moves:
        move.start()
    for move in moves:
        move.wait()
    _, where = peer_of(me, 1, devices, col_count)

    def first_exchange(pair, messages, group):
        return pltpu.make_async_remote_copy(
            src_ref=chunk.at[pair, pl.ds(0, messages)],
            dst_ref=chunk.at[pair, pl.ds(0, messages)],
            send_sem=send_sem,
            recv_sem=recv_sem.at[pair, group],
            device_id=where,
            device_id_type=MESH,
        )

    def aligned(at):
        return pl.multiple_of(at, few) if few % 8 == 0 else at

    lane_few = lax.broadcasted_iota(jnp.int32, (few, LANES), 1) // loads

    def unpack(pair, carry):
        for group in range(2):
            first_exchange(pair, near - 1 if group == 0 else near, group).wait_recv()

            def some(step, carry):
                for n in range(BATCH):
                    f = lax.rem(me + devices - (group * near + step * BATCH + n), devices)
                    parts_i = [chunk[pair, f, i * few : (i + 1) * few, :] for i in range(3)]
                    moved = [parts_i[0], pltpu.roll(parts_i[1], loads, 1), pltpu.roll(parts_i[2], 2 * loads, 1)]
                    for some_blocks in ((0, 3), (1, 4), (2, 5), (6,), (7,)):
                        second = functools.reduce(jnp.logical_or, [lane_few == (b + 1) % GROUP for b in some_blocks])
                        third = functools.reduce(jnp.logical_or, [lane_few == (b + 2) % GROUP for b in some_blocks])
                        mix = jnp.where(third, moved[2], jnp.where(second, moved[1], moved[0]))
                        for b in some_blocks:
                            line = pltpu.roll(mix, (LANES - b * loads) % LANES, 1) if b else mix
                            at = aligned(f * (GROUP * piece) + b * piece + pair * few)
                            table[pl.ds(at, few), :] = line
                return carry

            lax.fori_loop(0, near // BATCH, some, 0)
        return carry

    lax.fori_loop(0, pairs, unpack, 0)
    sent_all = pltpu.make_async_remote_copy(
        src_ref=chunk.at[:, pl.ds(0, devices - 1)],
        dst_ref=chunk.at[:, pl.ds(0, devices - 1)],
        send_sem=send_sem,
        recv_sem=recv_sem.at[0, 0],
        device_id=where,
        device_id_type=MESH,
    )
    sent_all.wait_send()

    span = lines * LANES

    def take(line, carry):
        for j in range(LANES):
            for n in range(SLOT_REFS):
                ordered[pl.ds(n * span + line * LANES + j, 1), :] = table[pl.ds(slots[n][line, j], 1), :]
        return carry

    lax.fori_loop(0, lines, take, 0)

    def turn(r, carry):
        turned = ordered[pl.ds(pl.multiple_of(r * LANES, LANES), LANES), :].T
        rhs[pl.ds(r, 3 * loads, stride=height), :] = turned[: 3 * loads, :]
        return carry

    lax.fori_loop(0, height, turn, 0, unroll=12)

    part_loads = loads // HALVES
    planes = 3 * part_loads
    exists = (row > 0, row < row_count - 1, col > 0, col < col_count - 1)
    peers = (
        {"row": row - 1, "col": col},
        {"row": row + 1, "col": col},
        {"row": row, "col": col - 1},
        {"row": row, "col": col + 1},
    )
    extent = (planes, planes, height, height)
    lane = lax.broadcasted_iota(jnp.int32, (height, LANES), 1)

    def plane_rows(index):
        return pl.ds(pl.multiple_of(index * height, height), height)

    def first(half):
        def one(q, carry):
            source = half * part_loads + q
            given = [rhs[plane_rows(j * loads + source), :] for j in range(3)]
            for i in range(3):
                total = inverse_ref[i, 0] * given[0]
                total = total + inverse_ref[i, 1] * given[1]
                total = total + inverse_ref[i, 2] * given[2]
                base[half * planes + i * part_loads + q] = total
                x[0, half * planes + i * part_loads + q, 8 : 8 + height, :] = total
            return carry

        lax.fori_loop(0, part_loads, one, 0, unroll=2)

    def pack(slot, step, half):
        own = slice(half * planes, (half + 1) * planes)
        edge[step, half, 0, :planes, :] = x[slot, own, 8, :]
        edge[step, half, 1, :planes, :] = x[slot, own, 7 + height, :]

        def columns(p, carry):
            left, right = carry
            plane = x[slot, half * planes + p, 8 : 8 + height, :]
            moved = pltpu.roll(plane, 2 * p + 1, 1)
            left = jnp.where(lane == 2 * p + 1, moved, left)
            right = jnp.where(lane == 2 * p, moved, right)
            return left, right

        blank = jnp.zeros((height, LANES), jnp.float32)
        left, right = lax.fori_loop(0, planes, columns, (blank, blank), unroll=12)
        edge[step, half, 2, :height, :] = left
        edge[step, half, 3, :height, :] = right

    def copy_edge(step, half, d, side):
        return pltpu.make_async_remote_copy(
            src_ref=edge.at[step, half, d, pl.ds(0, extent[d])],
            dst_ref=halo.at[step, half, side, pl.ds(0, extent[d])],
            send_sem=halo_send_sem.at[step, half, d],
            recv_sem=halo_recv_sem.at[step, half, side],
            device_id=peers[d],
            device_id_type=MESH,
        )

    def start(step, half):
        for d in range(4):

            @pl.when(exists[d])
            def _():
                copy_edge(step, half, d, d ^ 1).start()

    for half in range(HALVES):
        first(half)
        pack(0, 0, half)
        start(0, half)
    for step in range(ITERS - 1):
        old = step % 2
        last = step == ITERS - 2
        for half in range(HALVES):
            for d in range(4):

                @pl.when(exists[d])
                def _():
                    copy_edge(step, half, d, d).wait_send()
                    copy_edge(step, half, d, d).wait_recv()

            own = slice(half * planes, (half + 1) * planes)
            x[old, own, 7, :] = halo[step, half, 0, :planes, :]
            x[old, own, 8 + height, :] = halo[step, half, 1, :planes, :]
            sides = jnp.where(
                lane % 2 == 0,
                halo[step, half, 2, :height, :],
                pltpu.roll(halo[step, half, 3, :height, :], LANES - 2, 1),
            )
            both[half] = sides

            def update(q, carry):
                totals = [base[half * planes + i * part_loads + q] for i in range(3)]
                for k in range(3):
                    local = k * part_loads + q
                    p = half * planes + local
                    plane = x[old, p, 8 : 8 + height, :]
                    ends = pltpu.roll(both[half], lax.rem(LANES - 2 * local, LANES), 1)
                    left = jnp.where(lane == 0, ends, pltpu.roll(plane, 1, 1))
                    right = jnp.where(lane == LANES - 1, ends, pltpu.roll(plane, LANES - 1, 1))
                    shifted = (x[old, p, 7 : 7 + height, :], x[old, p, 9 : 9 + height, :], left, right)
                    for d in range(4):
                        for i in range(3):
                            totals[i] = totals[i] - mixed[d, i, k] * shifted[d]
                for i in range(3):
                    if last:
                        planes_ref[plane_rows(i * loads + half * part_loads + q), :] = totals[i]
                    else:
                        x[1 - old, half * planes + i * part_loads + q, 8 : 8 + height, :] = totals[i]
                return carry

            lax.fori_loop(0, part_loads, update, 0, unroll=2)
            if not last:
                pack(1 - old, step + 1, half)
                start(step + 1, half)

    out_copy = pltpu.make_async_copy(planes_ref, planes_hbm, small_sem.at[0])
    out_copy.start()

    def back(r, carry):
        plane = planes_ref[pl.ds(r, 3 * loads, stride=height), :]
        ordered[pl.ds(pl.multiple_of(r * LANES, LANES), LANES), : 3 * loads] = plane.T
        return carry

    lax.fori_loop(0, height, back, 0, unroll=12)
    lane_few = lax.broadcasted_iota(jnp.int32, (few, LANES), 1)

    def pack_back(pair, peer, at):
        for block in range(GROUP):
            for n in range(few):
                line = (pair * PAIR + n // parts) * GROUP + block
                source = places[line, (n % parts) * devices + peer]
                table[pl.ds(at + block * few + n, 1), :] = ordered[pl.ds(source, 1), :]
        lines = [table[at + block * few : at + (block + 1) * few, :] for block in range(GROUP)]
        results = []
        for i in range(3):
            result = None
            for block in range(GROUP):
                shift = ((block - i) * loads) % LANES
                moved = pltpu.roll(lines[block], shift, 1) if shift else lines[block]
                result = moved if result is None else jnp.where(lane_few < block * loads, result, moved)
            results.append(result)
        return results

    def place_of(pair, device):
        return (pair * devices + device) * rows

    def give_back(pair, carry):
        def give(step, carry):
            for n in range(2):
                index = 2 * step + 1 + n
                peer, where = peer_of(me, index, devices, col_count)
                results = pack_back(pair, peer, n * GROUP * few)
                for i in range(3):
                    packed[pl.ds(place_of(pair, peer) + i * few, few), :] = results[i]

                def send():
                    pltpu.make_async_remote_copy(
                        src_ref=packed.at[pl.ds(place_of(pair, peer), rows)],
                        dst_ref=arrived.at[pl.ds(place_of(pair, me), rows)],
                        send_sem=back_send_sem.at[pair],
                        recv_sem=back_recv_sem.at[pair],
                        device_id=where,
                        device_id_type=MESH,
                    ).start()

                if n == 0:
                    send()
                else:
                    pl.when(index < devices)(send)
            return carry

        lax.fori_loop(0, devices // 2, give, 0)
        arrived[pl.ds(place_of(pair, me), rows), :] = packed[pl.ds(place_of(pair, me), rows), :]
        return carry

    lax.fori_loop(0, pairs, give_back, 0)
    for pair in range(pairs):
        _, where = peer_of(me, 1, devices, col_count)
        every = pltpu.make_async_remote_copy(
            src_ref=packed.at[pl.ds(place_of(pair, 0), (devices - 1) * rows)],
            dst_ref=arrived.at[pl.ds(place_of(pair, 0), (devices - 1) * rows)],
            send_sem=back_send_sem.at[pair],
            recv_sem=back_recv_sem.at[pair],
            device_id=where,
            device_id_type=MESH,
        )
        every.wait_send()
        every.wait_recv()
        for i in range(3):
            for half in range(PAIR):
                at = place_of(pair, 0) + (i * PAIR + half) * parts
                pieces = [arrived[pl.ds(at + part, devices, stride=rows), :] for part in range(parts)]
                values[pair, i, half] = jnp.concatenate(pieces, axis=0).T if parts > 1 else pieces[0].T
        pltpu.make_async_copy(values.at[pair], values_hbm.at[pair], values_sem.at[pair]).start()
    out_copy.wait()
    for pair in range(pairs):
        pltpu.make_async_copy(values.at[pair], values_hbm.at[pair], values_sem.at[pair]).wait()


def main(cells, residual, restriction, present, inverse, blocks, pattern, row_count, col_count):
    loads = residual.shape[0]
    residual = residual.transpose(1, 0, 2)
    devices = row_count * col_count
    parts = LANES // devices
    width = LANES * GROUP * PAIR
    pairs = AGG_DEV // width
    present = present.reshape(-1, GROUP * PAIR, LANES)
    height = inverse.shape[2]
    rows = 3 * PAIR * parts
    planes = 3 * loads
    steps = ITERS - 1
    span = max(planes // HALVES, height)
    count = height * LANES
    blocks_own = AGG_DEV // LANES
    dma = pltpu.SemaphoreType.DMA
    scratch = [pltpu.SMEM((height // SLOT_REFS, LANES), jnp.int32) for _ in range(SLOT_REFS)]
    scratch += [
        pltpu.SMEM((blocks_own, LANES), jnp.int32),
        pltpu.VMEM((height, LANES), jnp.int32),
        pltpu.VMEM((height, LANES), jnp.int32),
        pltpu.VMEM((blocks_own, LANES), jnp.int32),
        pltpu.VMEM((2 * blocks_own, LANES), jnp.float32),
        pltpu.VMEM((2, height, LANES), jnp.float32),
        pltpu.VMEM((pairs, FPA, 3, loads, width), jnp.float32),
        pltpu.VMEM(restriction.shape, jnp.float32),
        pltpu.VMEM(present.shape, jnp.int32),
        pltpu.VMEM(inverse.shape, jnp.float32),
        pltpu.VMEM(blocks.shape, jnp.float32),
        pltpu.VMEM(pattern.shape, jnp.int32),
        pltpu.VMEM((3, LANES, LANES), jnp.float32),
        pltpu.VMEM((pairs * devices * rows, LANES), jnp.float32),
        pltpu.VMEM((pairs, devices, rows, LANES), jnp.float32),
        pltpu.VMEM((AGG_DEV, LANES), jnp.float32),
        pltpu.VMEM((count, LANES), jnp.float32),
        pltpu.VMEM((planes * height, LANES), jnp.float32),
        pltpu.VMEM((planes * height, LANES), jnp.float32),
        pltpu.VMEM((planes, height, LANES), jnp.float32),
        pltpu.VMEM((2, planes, height + 16, LANES), jnp.float32),
        pltpu.VMEM((4, 3, 3, height, LANES), jnp.float32),
        pltpu.VMEM((steps, HALVES, 4, span, LANES), jnp.float32),
        pltpu.VMEM((steps, HALVES, 4, span, LANES), jnp.float32),
        pltpu.VMEM((HALVES, height, LANES), jnp.float32),
        pltpu.VMEM((pairs * devices * rows, LANES), jnp.float32),
        pltpu.VMEM((pairs * devices * rows, LANES), jnp.float32),
        pltpu.VMEM((pairs, 3, PAIR, LANES, LANES), jnp.float32),
        dma((pairs + 1,)),
        dma((pairs + 1,)),
        dma((5,)),
        dma((SLOT_REFS,)),
        dma,
        dma((pairs, 2)),
        dma((steps, HALVES, 4)),
        dma((steps, HALVES, 4)),
        dma((pairs,)),
        dma((pairs,)),
        dma((pairs,)),
    ]
    return pl.pallas_call(
        functools.partial(main_kernel, row_count, col_count, loads),
        in_specs=[spec_any()] * 7,
        out_specs=(spec_any(), spec_any()),
        out_shape=(
            jax.ShapeDtypeStruct((pairs, 3, PAIR, LANES, LANES), jnp.float32),
            jax.ShapeDtypeStruct((planes * height, LANES), jnp.float32),
        ),
        scratch_shapes=scratch,
        compiler_params=pltpu.CompilerParams(vmem_limit_bytes=VMEM_LIMIT, collective_id=1, has_side_effects=True),
        name="correct",
    )(cells, residual, restriction, present, inverse, blocks, pattern)


def prolong_kernel(
    values_hbm,
    restriction_hbm,
    pattern_hbm,
    planes_hbm,
    out_hbm,
    iterate_hbm,
    values,
    restriction,
    pattern,
    planes,
    out,
    restriction_sem,
    small_sem,
    out_sem,
    iterate_sem,
):
    pairs = values.shape[0]
    loads = out.shape[1]
    blocks = AGG_DEV // LANES

    def slab(p):
        return pl.ds(pl.multiple_of(p * AGG_DEV, LANES), AGG_DEV)

    def restriction_copy(p):
        return pltpu.make_async_copy(restriction_hbm.at[:, :, slab(p)], restriction.at[:, :, slab(p)], restriction_sem.at[p])

    def out_copy(p):
        return pltpu.make_async_copy(out.at[:, :, slab(p)], out_hbm.at[:, :, slab(p)], out_sem.at[p])

    small = [
        pltpu.make_async_copy(pattern_hbm, pattern, small_sem.at[0]),
        pltpu.make_async_copy(values_hbm, values, small_sem.at[1]),
        pltpu.make_async_copy(planes_hbm, planes, small_sem.at[2]),
    ]
    small[1].start()
    restriction_copy(0).start()
    small[0].start()
    for p in range(1, FPA):
        restriction_copy(p).start()
    small[2].start()
    small[0].wait()
    small[1].wait()

    def one(p, carry):
        restriction_copy(p).wait()
        for b in range(blocks):
            pair, half, block = b // (GROUP * PAIR), b // GROUP % PAIR, b % GROUP
            lanes = pl.ds(pl.multiple_of(p * AGG_DEV + b * LANES, LANES), LANES)
            present = pattern[pl.ds(p * blocks + b, 1), :].astype(jnp.float32)
            terms = [values[pair, i, half, block * loads : (block + 1) * loads, :] * present for i in range(3)]
            for j in range(3):
                total = restriction[0, j : j + 1, lanes] * terms[0]
                total = total + restriction[1, j : j + 1, lanes] * terms[1]
                out[j, :, lanes] = total + restriction[2, j : j + 1, lanes] * terms[2]
        out_copy(p).start()
        return carry

    lax.fori_loop(0, FPA, one, 0)
    small[2].wait()
    turned = [pltpu.make_async_copy(planes.at[i], iterate_hbm.at[:, i], iterate_sem.at[i]) for i in range(3)]
    for copy in turned:
        copy.start()
    for copy in turned:
        copy.wait()
    for p in range(FPA):
        out_copy(p).wait()


def prolong(values, restriction, pattern, planes, loads, height):
    pattern = pattern.reshape(-1, LANES)
    planes = planes.reshape(3, loads, height, LANES)
    dma = pltpu.SemaphoreType.DMA
    shape = (3, loads, restriction.shape[2])
    out, iterate = pl.pallas_call(
        prolong_kernel,
        in_specs=[spec_any()] * 4,
        out_specs=(spec_any(), spec_any()),
        out_shape=(
            jax.ShapeDtypeStruct(shape, jnp.float32),
            jax.ShapeDtypeStruct((loads, 3, height, LANES), jnp.float32),
        ),
        scratch_shapes=[
            pltpu.VMEM(values.shape, jnp.float32),
            pltpu.VMEM(restriction.shape, jnp.float32),
            pltpu.VMEM(pattern.shape, jnp.int32),
            pltpu.VMEM(planes.shape, jnp.float32),
            pltpu.VMEM(shape, jnp.float32),
            dma((FPA,)),
            dma((3,)),
            dma((FPA,)),
            dma((3,)),
        ],
        compiler_params=pltpu.CompilerParams(vmem_limit_bytes=VMEM_LIMIT),
        name="prolong",
    )(values, restriction, pattern, planes)
    return out.transpose(1, 0, 2), iterate


def body(
    fine_residual,
    restriction,
    restriction_pattern,
    cell_aggregate,
    block_inverse,
    off_blocks,
    operator_pattern,
):
    loads = fine_residual.shape[0]
    row_count = lax.axis_size("row")
    col_count = lax.axis_size("col")
    height = cell_aggregate.shape[0]
    values, planes = main(
        cell_aggregate,
        fine_residual,
        restriction,
        restriction_pattern,
        block_inverse,
        off_blocks,
        operator_pattern,
        row_count,
        col_count,
    )
    fine_correction, iterate = prolong(values, restriction, restriction_pattern, planes, loads, height)
    return (iterate, fine_correction)


def solution(mesh):
    in_specs = (
        P(None, None, ("row", "col")),
        P(None, None, ("row", "col")),
        P(("row", "col")),
        P("row", "col"),
        P(None, None, "row", "col"),
        P(None, None, None, "row", "col"),
        P(None, "row", "col"),
    )
    out_specs = (P(None, None, "row", "col"), P(None, None, ("row", "col")))
    return jax.shard_map(body, mesh=mesh, in_specs=in_specs, out_specs=out_specs, check_vma=False)
```

```python
import functools

import jax
import jax.numpy as jnp
from jax import lax
from jax.experimental import pallas as pl
from jax.experimental.pallas import tpu as pltpu
from jax.sharding import PartitionSpec as P

FPA = 8
ITERS = 4
AGG_DEV = 6144
LANES = 128
GROUP = 8
PAIR = 2
HALVES = 4
BATCH = 8
SLOT_REFS = 6
MESH = pl.DeviceIdType.MESH
VMEM_LIMIT = 56 * 1024 * 1024


def spec_vmem():
    return pl.BlockSpec(memory_space=pltpu.VMEM)


def spec_any():
    return pl.BlockSpec(memory_space=pl.ANY)


def peer_of(me, index, devices, col_count):
    peer = lax.rem(me + index, devices)
    return peer, {"row": peer // col_count, "col": lax.rem(peer, col_count)}


def greet(devices, col_count, me):
    barrier = pltpu.get_barrier_semaphore()

    def signal(index, carry):
        _, where = peer_of(me, index, devices, col_count)
        pl.semaphore_signal(barrier, inc=1, device_id=where, device_id_type=MESH)
        return carry

    lax.fori_loop(1, devices, signal, 0)
    return barrier


def fill_tables(devices, cells_ref, slots_ref, inverse_ref, total_ref, owner_ref):
    height = cells_ref.shape[0]
    parts = LANES // devices
    blocks = AGG_DEV // LANES
    piece = blocks * parts // GROUP
    value = cells_ref[...].astype(jnp.float32)
    owner = jnp.floor((value + 0.5) * (1.0 / AGG_DEV))
    inside = value - owner * AGG_DEV
    block = jnp.floor((inside + 0.5) * (1.0 / LANES))
    part = jnp.floor((inside - block * LANES + 0.5) * (1.0 / devices))
    group = jnp.floor((block + 0.5) * (1.0 / GROUP))
    slot = owner * (GROUP * piece) + (block - group * GROUP) * piece + group * parts + part
    slots_ref[...] = jnp.clip(slot.astype(jnp.int32), 0, AGG_DEV - 1)
    owner_ref[0] = block
    owner_ref[1] = part * devices + owner
    rows = lax.broadcasted_iota(jnp.int32, (blocks, LANES), 0).astype(jnp.float32)
    lanes = lax.broadcasted_iota(jnp.int32, (blocks, LANES), 1).astype(jnp.float32)
    places = lax.broadcasted_iota(jnp.int32, (LANES, LANES), 0).astype(jnp.float32)
    total_ref[...] = jnp.zeros_like(total_ref)

    def some(r, carry):
        hit = rows == owner_ref[0, pl.ds(r, 1), :]
        low = jnp.where(hit, lanes, 0.0)
        high = jnp.where(hit, r.astype(jnp.float32), 0.0)
        left = jnp.concatenate([low, high], axis=0).astype(jnp.bfloat16)
        right = jnp.where(places == owner_ref[1, pl.ds(r, 1), :], 1.0, 0.0).astype(jnp.bfloat16)
        total_ref[...] += lax.dot_general(left, right, (((1,), (1,)), ((), ())), preferred_element_type=jnp.float32)
        return carry

    lax.fori_loop(0, height, some, 0, unroll=4)
    inverse = (total_ref[:blocks] + total_ref[blocks:] * LANES).astype(jnp.int32)
    inverse_ref[...] = jnp.clip(inverse, 0, height * LANES - 1)


def main_kernel(row_count, col_count, loads, *refs):
    (
        cells_hbm,
        residual_hbm,
        restriction_hbm,
        present_hbm,
        inverse_hbm,
        blocks_hbm,
        pattern_hbm,
        values_hbm,
        last_hbm,
        planes_hbm,
    ) = refs[:10]
    slots = refs[10 : 10 + SLOT_REFS]
    (
        places,
        cells,
        slots_all,
        places_all,
        total,
        digits,
        residual,
        restriction,
        present_all,
        inverse_ref,
        blocks_ref,
        pattern_ref,
        stage,
        sent,
        chunk,
        table,
        ordered,
        rhs,
        planes_ref,
        base,
        x,
        mixed,
        edge,
        halo,
        both,
        sides,
        ends_in,
        packed,
        arrived,
        values,
        residual_sem,
        restriction_sem,
        small_sem,
        slots_sem,
        send_sem,
        recv_sem,
        halo_send_sem,
        halo_recv_sem,
        back_send_sem,
        back_recv_sem,
        values_sem,
    ) = refs[10 + SLOT_REFS :]
    devices = row_count * col_count
    parts = LANES // devices
    pairs = residual.shape[0]
    width = residual.shape[-1]
    height = inverse_ref.shape[2]
    few = PAIR * parts
    piece = pairs * few
    row = lax.axis_index("row")
    col = lax.axis_index("col")
    me = row * col_count + col
    rows = 3 * few
    half_width = width // PAIR
    small = [
        pltpu.make_async_copy(present_hbm, present_all, small_sem.at[0]),
        pltpu.make_async_copy(cells_hbm, cells, small_sem.at[1]),
        pltpu.make_async_copy(inverse_hbm, inverse_ref, small_sem.at[2]),
        pltpu.make_async_copy(blocks_hbm, blocks_ref, small_sem.at[3]),
        pltpu.make_async_copy(pattern_hbm, pattern_ref, small_sem.at[4]),
    ]

    def load(pair, first_lane, count, which):
        for p in range(FPA):
            lanes = pl.ds((p * pairs + pair) * width + first_lane, count)
            target = residual.at[pair, p, :, :, pl.ds(first_lane, count)]
            pltpu.make_async_copy(residual_hbm.at[:, :, lanes], target, residual_sem.at[which]).start()
            target = restriction.at[:, :, lanes]
            pltpu.make_async_copy(restriction_hbm.at[:, :, lanes], target, restriction_sem.at[which]).start()

    def loaded(pair, first_lane, count, which):
        target = residual.at[pair, :, :, :, pl.ds(first_lane, count)]
        pltpu.make_async_copy(target, target, residual_sem.at[which]).wait()
        target = restriction.at[:, :, pl.ds(0, FPA * count)]
        pltpu.make_async_copy(target, target, restriction_sem.at[which]).wait()

    small[0].start()
    load(0, 0, half_width, 0)
    load(0, half_width, half_width, pairs)
    barrier = greet(devices, col_count, me)
    for pair in range(1, pairs):
        load(pair, 0, width, pair)
    for copy in small[1:]:
        copy.start()
    halo[...] = jnp.zeros_like(halo)
    edge[...] = jnp.zeros_like(edge)
    ends_in[...] = jnp.zeros_like(ends_in)
    both[...] = jnp.zeros_like(both)
    small[0].wait()

    near = devices // 2

    def send_first(pair):
        def send(index, carry):
            peer, where = peer_of(me, index, devices, col_count)
            pltpu.make_async_remote_copy(
                src_ref=sent.at[pl.ds((pair * devices + peer) * rows, rows)],
                dst_ref=chunk.at[pair, me],
                send_sem=send_sem,
                recv_sem=recv_sem.at[pair, index // near],
                device_id=where,
                device_id_type=MESH,
            ).start()
            return carry

        lax.fori_loop(1, devices, send, 0)

    def restrict(pair, split):
        if not split:
            loaded(pair, 0, width, pair)
        for half in range(PAIR):
            if split:
                loaded(pair, half * half_width, half_width, pairs if half else 0)
            for block in range(GROUP):
                start = (half * GROUP + block) * LANES
                lanes = slice(start, start + LANES)
                which = half * GROUP + block
                totals = [None, None, None]
                for p in range(FPA):
                    there = pl.ds(pl.multiple_of((p * pairs + pair) * width + start, LANES), LANES)
                    present = present_all[p * pairs + pair, which : which + 1, :].astype(jnp.float32)
                    for j in range(3):
                        masked = residual[pair, p, j, :, lanes] * present
                        for i in range(3):
                            term = restriction[i, j : j + 1, there] * masked
                            totals[i] = term if totals[i] is None else totals[i] + term
                for i in range(3):
                    stage[i, block * loads : (block + 1) * loads, :] = totals[i]
            for i in range(3):
                turned = stage[i].T
                for part in range(parts):
                    at = pair * (devices * rows) + (i * PAIR + half) * parts + part
                    sent[pl.ds(at, devices, stride=rows), :] = turned[part * devices : (part + 1) * devices, :]

    restrict(0, True)
    pl.semaphore_wait(barrier, devices - 1)
    send_first(0)

    def later(pair, carry):
        restrict(pair, False)
        send_first(pair)
        return carry

    lax.fori_loop(1, pairs, later, 0)
    for copy in small[1:]:
        copy.wait()

    def keep(pair, carry):
        chunk[pair, me] = sent[pl.ds((pair * devices + me) * rows, rows), :]
        return carry

    lax.fori_loop(0, pairs, keep, 0)

    def fold(d, carry):
        on = pattern_ref[d].astype(jnp.float32)
        for k in range(3):
            column = [blocks_ref[d, j, k] * on for j in range(3)]
            for i in range(3):
                total = inverse_ref[i, 0] * column[0]
                total = total + inverse_ref[i, 1] * column[1]
                mixed[d, i, k] = total + inverse_ref[i, 2] * column[2]
        return carry

    lax.fori_loop(0, 4, fold, 0)
    fill_tables(devices, cells, slots_all, places_all, total, digits)
    lines = slots[0].shape[0]
    moves = [pltpu.make_async_copy(places_all, places, small_sem.at[0])]
    for n in range(SLOT_REFS):
        moves.append(pltpu.make_async_copy(slots_all.at[pl.ds(n * lines, lines)], slots[n], slots_sem.at[n]))
    for move in moves:
        move.start()
    for move in moves:
        move.wait()
    _, where = peer_of(me, 1, devices, col_count)

    def first_exchange(pair, messages, group):
        return pltpu.make_async_remote_copy(
            src_ref=chunk.at[pair, pl.ds(0, messages)],
            dst_ref=chunk.at[pair, pl.ds(0, messages)],
            send_sem=send_sem,
            recv_sem=recv_sem.at[pair, group],
            device_id=where,
            device_id_type=MESH,
        )

    def aligned(at):
        return pl.multiple_of(at, few) if few % 8 == 0 else at

    lane_few = lax.broadcasted_iota(jnp.int32, (few, LANES), 1) // loads

    def unpack(pair, carry):
        for group in range(2):
            first_exchange(pair, near - 1 if group == 0 else near, group).wait_recv()

            def some(step, carry):
                for n in range(BATCH):
                    f = lax.rem(me + devices - (group * near + step * BATCH + n), devices)
                    parts_i = [chunk[pair, f, i * few : (i + 1) * few, :] for i in range(3)]
                    moved = [parts_i[0], pltpu.roll(parts_i[1], loads, 1), pltpu.roll(parts_i[2], 2 * loads, 1)]
                    for some_blocks in ((0, 3), (1, 4), (2, 5), (6,), (7,)):
                        second = functools.reduce(jnp.logical_or, [lane_few == (b + 1) % GROUP for b in some_blocks])
                        third = functools.reduce(jnp.logical_or, [lane_few == (b + 2) % GROUP for b in some_blocks])
                        mix = jnp.where(third, moved[2], jnp.where(second, moved[1], moved[0]))
                        for b in some_blocks:
                            line = pltpu.roll(mix, (LANES - b * loads) % LANES, 1) if b else mix
                            at = aligned(f * (GROUP * piece) + b * piece + pair * few)
                            table[pl.ds(at, few), :] = line
                return carry

            lax.fori_loop(0, near // BATCH, some, 0)
        return carry

    lax.fori_loop(0, pairs, unpack, 0)
    sent_all = pltpu.make_async_remote_copy(
        src_ref=chunk.at[:, pl.ds(0, devices - 1)],
        dst_ref=chunk.at[:, pl.ds(0, devices - 1)],
        send_sem=send_sem,
        recv_sem=recv_sem.at[0, 0],
        device_id=where,
        device_id_type=MESH,
    )
    sent_all.wait_send()

    span = lines * LANES

    def take(line, carry):
        for j in range(LANES):
            for n in range(SLOT_REFS):
                ordered[pl.ds(n * span + line * LANES + j, 1), :] = table[pl.ds(slots[n][line, j], 1), :]
        return carry

    lax.fori_loop(0, lines, take, 0)

    def turn(r, carry):
        turned = ordered[pl.ds(pl.multiple_of(r * LANES, LANES), LANES), :].T
        rhs[pl.ds(r, 3 * loads, stride=height), :] = turned[: 3 * loads, :]
        return carry

    lax.fori_loop(0, height, turn, 0, unroll=12)

    part_loads = loads // HALVES
    planes = 3 * part_loads
    end_rows = ends_in.shape[1]
    exists = (row > 0, row < row_count - 1, col > 0, col < col_count - 1)
    peers = (
        {"row": row - 1, "col": col},
        {"row": row + 1, "col": col},
        {"row": row, "col": col - 1},
        {"row": row, "col": col + 1},
    )
    lane = lax.broadcasted_iota(jnp.int32, (height, LANES), 1)

    def plane_rows(index):
        return pl.ds(pl.multiple_of(index * height, height), height)

    def first(half):
        def one(q, carry):
            source = half * part_loads + q
            given = [rhs[plane_rows(j * loads + source), :] for j in range(3)]
            for i in range(3):
                total = inverse_ref[i, 0] * given[0]
                total = total + inverse_ref[i, 1] * given[1]
                total = total + inverse_ref[i, 2] * given[2]
                base[half * planes + i * part_loads + q] = total
                x[0, half * planes + i * part_loads + q, 8 : 8 + height, :] = total
            return carry

        lax.fori_loop(0, part_loads, one, 0, unroll=2)

    def pack(slot, step, half):
        own = slice(half * planes, (half + 1) * planes)
        edge[step, half, 0] = x[slot, own, 8, :]
        edge[step, half, 1] = x[slot, own, 7 + height, :]

        def columns(p, mix):
            moved = pltpu.roll(x[slot, half * planes + p, 8 : 8 + height, :], 2 * p + 1, 1)
            return jnp.where(lane // 2 == p, moved, mix)

        mix = lax.fori_loop(0, planes, columns, jnp.zeros((height, LANES), jnp.float32), unroll=12)
        sides[half, : 2 * planes, :height] = mix.T[: 2 * planes]
        edge[step, half, 2, :, :height] = sides[half, pl.ds(1, planes, stride=2), :height]
        edge[step, half, 3, :, :height] = sides[half, pl.ds(0, planes, stride=2), :height]

    def copy_edge(step, half, d, side):
        return pltpu.make_async_remote_copy(
            src_ref=edge.at[step, half, d],
            dst_ref=halo.at[step, half, side],
            send_sem=halo_send_sem.at[step, half, d],
            recv_sem=halo_recv_sem.at[step, half, side],
            device_id=peers[d],
            device_id_type=MESH,
        )

    def start(step, half):
        for d in range(4):

            @pl.when(exists[d])
            def _():
                copy_edge(step, half, d, d ^ 1).start()

    for half in range(HALVES):
        first(half)
        pack(0, 0, half)
        start(0, half)
    for step in range(ITERS - 1):
        old = step % 2
        last = step == ITERS - 2
        for half in range(HALVES):
            for d in range(4):

                @pl.when(exists[d])
                def _():
                    copy_edge(step, half, d, d).wait_send()
                    copy_edge(step, half, d, d).wait_recv()

            own = slice(half * planes, (half + 1) * planes)
            x[old, own, 7, :] = halo[step, half, 0]
            x[old, own, 8 + height, :] = halo[step, half, 1]
            ends_in[half, pl.ds(2, planes, stride=2), :] = halo[step, half, 2]
            ends_in[half, pl.ds(1, planes, stride=2), :] = halo[step, half, 3]
            both[half, :, :end_rows] = ends_in[half].T[:height]

            def update(q, carry):
                totals = [base[half * planes + i * part_loads + q] for i in range(3)]
                for k in range(3):
                    local = k * part_loads + q
                    p = half * planes + local
                    plane = x[old, p, 8 : 8 + height, :]
                    ends = pltpu.roll(both[half], LANES - 2 - 2 * local, 1)
                    left = jnp.where(lane == 0, ends, pltpu.roll(plane, 1, 1))
                    right = jnp.where(lane == LANES - 1, ends, pltpu.roll(plane, LANES - 1, 1))
                    shifted = (x[old, p, 7 : 7 + height, :], x[old, p, 9 : 9 + height, :], left, right)
                    for d in range(4):
                        for i in range(3):
                            totals[i] = totals[i] - mixed[d, i, k] * shifted[d]
                for i in range(3):
                    if last:
                        planes_ref[plane_rows(i * loads + half * part_loads + q), :] = totals[i]
                    else:
                        x[1 - old, half * planes + i * part_loads + q, 8 : 8 + height, :] = totals[i]
                return carry

            lax.fori_loop(0, part_loads, update, 0, unroll=2)
            if not last:
                pack(1 - old, step + 1, half)
                start(step + 1, half)

    out_copy = pltpu.make_async_copy(planes_ref, planes_hbm, small_sem.at[0])
    out_copy.start()

    def back(r, carry):
        plane = planes_ref[pl.ds(r, 3 * loads, stride=height), :]
        ordered[pl.ds(pl.multiple_of(r * LANES, LANES), LANES), : 3 * loads] = plane.T
        return carry

    lax.fori_loop(0, height, back, 0, unroll=12)
    lane_few = lax.broadcasted_iota(jnp.int32, (few, LANES), 1)

    def pack_back(pair, peer, at):
        for block in range(GROUP):
            for n in range(few):
                line = (pair * PAIR + n // parts) * GROUP + block
                source = places[line, (n % parts) * devices + peer]
                table[pl.ds(at + block * few + n, 1), :] = ordered[pl.ds(source, 1), :]
        lines = [table[at + block * few : at + (block + 1) * few, :] for block in range(GROUP)]
        results = []
        for i in range(3):
            result = None
            for block in range(GROUP):
                shift = ((block - i) * loads) % LANES
                moved = pltpu.roll(lines[block], shift, 1) if shift else lines[block]
                result = moved if result is None else jnp.where(lane_few < block * loads, result, moved)
            results.append(result)
        return results

    def place_of(pair, device):
        return (pair * devices + device) * rows

    def give_back(pair, final):
        def give(step, carry):
            for n in range(2):
                index = 2 * step + 1 + n
                peer, where = peer_of(me, index, devices, col_count)
                results = pack_back(pair, peer, n * GROUP * few)
                for i in range(3):
                    packed[pl.ds(place_of(pair, peer) + i * few, few), :] = results[i]

                def send():
                    target = last_hbm.at[me] if final else arrived.at[pl.ds(place_of(pair, me), rows)]
                    pltpu.make_async_remote_copy(
                        src_ref=packed.at[pl.ds(place_of(pair, peer), rows)],
                        dst_ref=target,
                        send_sem=back_send_sem.at[pair],
                        recv_sem=back_recv_sem.at[pair],
                        device_id=where,
                        device_id_type=MESH,
                    ).start()

                if n == 0:
                    send()
                else:
                    pl.when(index < devices)(send)
            return carry

        lax.fori_loop(0, devices // 2, give, 0)
        if not final:
            arrived[pl.ds(place_of(pair, me), rows), :] = packed[pl.ds(place_of(pair, me), rows), :]

    def give_early(pair, carry):
        give_back(pair, False)
        return carry

    final = pairs - 1
    lax.fori_loop(0, final, give_early, 0)
    give_back(final, True)
    own = pltpu.make_async_copy(packed.at[pl.ds(place_of(final, me), rows)], last_hbm.at[me], values_sem.at[final])
    own.start()
    for pair in range(final):
        _, where = peer_of(me, 1, devices, col_count)
        every = pltpu.make_async_remote_copy(
            src_ref=packed.at[pl.ds(place_of(pair, 0), (devices - 1) * rows)],
            dst_ref=arrived.at[pl.ds(place_of(pair, 0), (devices - 1) * rows)],
            send_sem=back_send_sem.at[pair],
            recv_sem=back_recv_sem.at[pair],
            device_id=where,
            device_id_type=MESH,
        )
        every.wait_send()
        every.wait_recv()
        for i in range(3):
            for half in range(PAIR):
                at = place_of(pair, 0) + (i * PAIR + half) * parts
                pieces = [arrived[pl.ds(at + part, devices, stride=rows), :] for part in range(parts)]
                values[pair, i, half] = jnp.concatenate(pieces, axis=0).T if parts > 1 else pieces[0].T
        pltpu.make_async_copy(values.at[pair], values_hbm.at[pair], values_sem.at[pair]).start()
    out_copy.wait()
    own.wait()
    for pair in range(final):
        pltpu.make_async_copy(values.at[pair], values_hbm.at[pair], values_sem.at[pair]).wait()
    _, where = peer_of(me, 1, devices, col_count)
    every = pltpu.make_async_remote_copy(
        src_ref=last_hbm.at[pl.ds(0, devices - 1)],
        dst_ref=last_hbm.at[pl.ds(0, devices - 1)],
        send_sem=back_send_sem.at[final],
        recv_sem=back_recv_sem.at[final],
        device_id=where,
        device_id_type=MESH,
    )
    every.wait_send()
    every.wait_recv()


def main(cells, residual, restriction, present, inverse, blocks, pattern, row_count, col_count):
    loads = residual.shape[0]
    residual = residual.transpose(1, 0, 2)
    devices = row_count * col_count
    parts = LANES // devices
    width = LANES * GROUP * PAIR
    pairs = AGG_DEV // width
    present = present.reshape(-1, GROUP * PAIR, LANES)
    height = inverse.shape[2]
    rows = 3 * PAIR * parts
    planes = 3 * loads
    steps = ITERS - 1
    part_planes = planes // HALVES
    end_rows = -(-(2 * part_planes + 2) // 8) * 8
    count = height * LANES
    blocks_own = AGG_DEV // LANES
    dma = pltpu.SemaphoreType.DMA
    scratch = [pltpu.SMEM((height // SLOT_REFS, LANES), jnp.int32) for _ in range(SLOT_REFS)]
    scratch += [
        pltpu.SMEM((blocks_own, LANES), jnp.int32),
        pltpu.VMEM((height, LANES), jnp.int32),
        pltpu.VMEM((height, LANES), jnp.int32),
        pltpu.VMEM((blocks_own, LANES), jnp.int32),
        pltpu.VMEM((2 * blocks_own, LANES), jnp.float32),
        pltpu.VMEM((2, height, LANES), jnp.float32),
        pltpu.VMEM((pairs, FPA, 3, loads, width), jnp.float32),
        pltpu.VMEM(restriction.shape, jnp.float32),
        pltpu.VMEM(present.shape, jnp.int32),
        pltpu.VMEM(inverse.shape, jnp.float32),
        pltpu.VMEM(blocks.shape, jnp.float32),
        pltpu.VMEM(pattern.shape, jnp.int32),
        pltpu.VMEM((3, LANES, LANES), jnp.float32),
        pltpu.VMEM((pairs * devices * rows, LANES), jnp.float32),
        pltpu.VMEM((pairs, devices, rows, LANES), jnp.float32),
        pltpu.VMEM((AGG_DEV, LANES), jnp.float32),
        pltpu.VMEM((count, LANES), jnp.float32),
        pltpu.VMEM((planes * height, LANES), jnp.float32),
        pltpu.VMEM((planes * height, LANES), jnp.float32),
        pltpu.VMEM((planes, height, LANES), jnp.float32),
        pltpu.VMEM((2, planes, height + 16, LANES), jnp.float32),
        pltpu.VMEM((4, 3, 3, height, LANES), jnp.float32),
        pltpu.VMEM((steps, HALVES, 4, part_planes, LANES), jnp.float32),
        pltpu.VMEM((steps, HALVES, 4, part_planes, LANES), jnp.float32),
        pltpu.VMEM((HALVES, height, LANES), jnp.float32),
        pltpu.VMEM((HALVES, end_rows, LANES), jnp.float32),
        pltpu.VMEM((HALVES, end_rows, LANES), jnp.float32),
        pltpu.VMEM((pairs * devices * rows, LANES), jnp.float32),
        pltpu.VMEM(((pairs - 1) * devices * rows, LANES), jnp.float32),
        pltpu.VMEM((pairs - 1, 3, PAIR, LANES, LANES), jnp.float32),
        dma((pairs + 1,)),
        dma((pairs + 1,)),
        dma((5,)),
        dma((SLOT_REFS,)),
        dma,
        dma((pairs, 2)),
        dma((steps, HALVES, 4)),
        dma((steps, HALVES, 4)),
        dma((pairs,)),
        dma((pairs,)),
        dma((pairs,)),
    ]
    return pl.pallas_call(
        functools.partial(main_kernel, row_count, col_count, loads),
        in_specs=[spec_any()] * 7,
        out_specs=(spec_any(), spec_any(), spec_any()),
        out_shape=(
            jax.ShapeDtypeStruct((pairs - 1, 3, PAIR, LANES, LANES), jnp.float32),
            jax.ShapeDtypeStruct((devices, rows, LANES), jnp.float32),
            jax.ShapeDtypeStruct((planes * height, LANES), jnp.float32),
        ),
        scratch_shapes=scratch,
        compiler_params=pltpu.CompilerParams(vmem_limit_bytes=VMEM_LIMIT, collective_id=1, has_side_effects=True),
        name="correct",
    )(cells, residual, restriction, present, inverse, blocks, pattern)


def prolong_kernel(
    devices,
    values_hbm,
    last_hbm,
    restriction_hbm,
    pattern_hbm,
    planes_hbm,
    out_hbm,
    iterate_hbm,
    values,
    last,
    restriction,
    pattern,
    planes,
    out,
    restriction_sem,
    small_sem,
    out_sem,
    iterate_sem,
):
    final = values.shape[0] - 1
    parts = LANES // devices
    rows = last.shape[0] // devices
    loads = out.shape[1]
    blocks = AGG_DEV // LANES

    def slab(p):
        return pl.ds(pl.multiple_of(p * AGG_DEV, LANES), AGG_DEV)

    def restriction_copy(p):
        return pltpu.make_async_copy(restriction_hbm.at[:, :, slab(p)], restriction.at[:, :, slab(p)], restriction_sem.at[p])

    def out_copy(p):
        return pltpu.make_async_copy(out.at[:, :, slab(p)], out_hbm.at[:, :, slab(p)], out_sem.at[p])

    small = [
        pltpu.make_async_copy(pattern_hbm, pattern, small_sem.at[0]),
        pltpu.make_async_copy(values_hbm, values.at[pl.ds(0, final)], small_sem.at[1]),
        pltpu.make_async_copy(last_hbm, last, small_sem.at[3]),
        pltpu.make_async_copy(planes_hbm, planes, small_sem.at[2]),
    ]
    small[2].start()
    small[1].start()
    small[0].start()
    for p in range(FPA):
        restriction_copy(p).start()
    small[3].start()
    small[2].wait()
    for i in range(3):
        for half in range(PAIR):
            at = (i * PAIR + half) * parts
            pieces = [last[pl.ds(at + part, devices, stride=rows), :] for part in range(parts)]
            values[final, i, half] = jnp.concatenate(pieces, axis=0).T if parts > 1 else pieces[0].T
    small[0].wait()
    small[1].wait()

    def one(p, carry):
        restriction_copy(p).wait()
        for b in range(blocks):
            pair, half, block = b // (GROUP * PAIR), b // GROUP % PAIR, b % GROUP
            lanes = pl.ds(pl.multiple_of(p * AGG_DEV + b * LANES, LANES), LANES)
            present = pattern[pl.ds(p * blocks + b, 1), :].astype(jnp.float32)
            terms = [values[pair, i, half, block * loads : (block + 1) * loads, :] * present for i in range(3)]
            for j in range(3):
                total = restriction[0, j : j + 1, lanes] * terms[0]
                total = total + restriction[1, j : j + 1, lanes] * terms[1]
                out[j, :, lanes] = total + restriction[2, j : j + 1, lanes] * terms[2]
        out_copy(p).start()
        return carry

    lax.fori_loop(0, FPA, one, 0)
    small[3].wait()
    turned = [pltpu.make_async_copy(planes.at[i], iterate_hbm.at[:, i], iterate_sem.at[i]) for i in range(3)]
    for copy in turned:
        copy.start()
    for copy in turned:
        copy.wait()
    for p in range(FPA):
        out_copy(p).wait()


def prolong(values, last, restriction, pattern, planes, loads, height):
    pattern = pattern.reshape(-1, LANES)
    planes = planes.reshape(3, loads, height, LANES)
    devices = last.shape[0]
    last = last.reshape(-1, LANES)
    dma = pltpu.SemaphoreType.DMA
    shape = (3, loads, restriction.shape[2])
    out, iterate = pl.pallas_call(
        functools.partial(prolong_kernel, devices),
        in_specs=[spec_any()] * 5,
        out_specs=(spec_any(), spec_any()),
        out_shape=(
            jax.ShapeDtypeStruct(shape, jnp.float32),
            jax.ShapeDtypeStruct((loads, 3, height, LANES), jnp.float32),
        ),
        scratch_shapes=[
            pltpu.VMEM((values.shape[0] + 1,) + values.shape[1:], jnp.float32),
            pltpu.VMEM(last.shape, jnp.float32),
            pltpu.VMEM(restriction.shape, jnp.float32),
            pltpu.VMEM(pattern.shape, jnp.int32),
            pltpu.VMEM(planes.shape, jnp.float32),
            pltpu.VMEM(shape, jnp.float32),
            dma((FPA,)),
            dma((4,)),
            dma((FPA,)),
            dma((3,)),
        ],
        compiler_params=pltpu.CompilerParams(vmem_limit_bytes=VMEM_LIMIT),
        name="prolong",
    )(values, last, restriction, pattern, planes)
    return out.transpose(1, 0, 2), iterate


def body(
    fine_residual,
    restriction,
    restriction_pattern,
    cell_aggregate,
    block_inverse,
    off_blocks,
    operator_pattern,
):
    loads = fine_residual.shape[0]
    row_count = lax.axis_size("row")
    col_count = lax.axis_size("col")
    height = cell_aggregate.shape[0]
    values, last, planes = main(
        cell_aggregate,
        fine_residual,
        restriction,
        restriction_pattern,
        block_inverse,
        off_blocks,
        operator_pattern,
        row_count,
        col_count,
    )
    fine_correction, iterate = prolong(values, last, restriction, restriction_pattern, planes, loads, height)
    return (iterate, fine_correction)


def solution(mesh):
    in_specs = (
        P(None, None, ("row", "col")),
        P(None, None, ("row", "col")),
        P(("row", "col")),
        P("row", "col"),
        P(None, None, "row", "col"),
        P(None, None, None, "row", "col"),
        P(None, "row", "col"),
    )
    out_specs = (P(None, None, "row", "col"), P(None, None, ("row", "col")))
    return jax.shard_map(body, mesh=mesh, in_specs=in_specs, out_specs=out_specs, check_vma=False)
```

```python
import functools

import jax
import jax.numpy as jnp
from jax import lax
from jax.experimental import pallas as pl
from jax.experimental.pallas import tpu as pltpu
from jax.sharding import PartitionSpec as P

FPA = 8
ITERS = 4
AGG_DEV = 6144
LANES = 128
GROUP = 8
PAIR = 2
HALVES = 4
BATCH = 8
SLOT_REFS = 6
MESH = pl.DeviceIdType.MESH
VMEM_LIMIT = 56 * 1024 * 1024


def spec_vmem():
    return pl.BlockSpec(memory_space=pltpu.VMEM)


def spec_any():
    return pl.BlockSpec(memory_space=pl.ANY)


def peer_of(me, index, devices, col_count):
    peer = lax.rem(me + index, devices)
    return peer, {"row": lax.div(peer, col_count), "col": lax.rem(peer, col_count)}


def greet(devices, col_count, me):
    barrier = pltpu.get_barrier_semaphore()

    def signal(index, carry):
        _, where = peer_of(me, index, devices, col_count)
        pl.semaphore_signal(barrier, inc=1, device_id=where, device_id_type=MESH)
        return carry

    lax.fori_loop(1, devices, signal, 0)
    return barrier


def fill_tables(devices, cells_ref, slots_ref, inverse_ref, total_ref, owner_ref):
    height = cells_ref.shape[0]
    parts = LANES // devices
    blocks = AGG_DEV // LANES
    piece = blocks * parts // GROUP
    value = cells_ref[...].astype(jnp.float32)
    owner = jnp.floor((value + 0.5) * (1.0 / AGG_DEV))
    inside = value - owner * AGG_DEV
    block = jnp.floor((inside + 0.5) * (1.0 / LANES))
    part = jnp.floor((inside - block * LANES + 0.5) * (1.0 / devices))
    group = jnp.floor((block + 0.5) * (1.0 / GROUP))
    slot = owner * (GROUP * piece) + (block - group * GROUP) * piece + group * parts + part
    slots_ref[...] = jnp.clip(slot.astype(jnp.int32), 0, AGG_DEV - 1)
    owner_ref[0] = block
    owner_ref[1] = part * devices + owner
    rows = lax.broadcasted_iota(jnp.int32, (blocks, LANES), 0).astype(jnp.float32)
    lanes = lax.broadcasted_iota(jnp.int32, (blocks, LANES), 1).astype(jnp.float32)
    places = lax.broadcasted_iota(jnp.int32, (LANES, LANES), 0).astype(jnp.float32)
    total_ref[...] = jnp.zeros_like(total_ref)

    def some(r, carry):
        hit = rows == owner_ref[0, pl.ds(r, 1), :]
        low = jnp.where(hit, lanes, 0.0)
        high = jnp.where(hit, r.astype(jnp.float32), 0.0)
        left = jnp.concatenate([low, high], axis=0).astype(jnp.bfloat16)
        right = jnp.where(places == owner_ref[1, pl.ds(r, 1), :], 1.0, 0.0).astype(jnp.bfloat16)
        total_ref[...] += lax.dot_general(left, right, (((1,), (1,)), ((), ())), preferred_element_type=jnp.float32)
        return carry

    lax.fori_loop(0, height, some, 0, unroll=4)
    inverse = (total_ref[:blocks] + total_ref[blocks:] * LANES).astype(jnp.int32)
    inverse_ref[...] = jnp.clip(inverse, 0, height * LANES - 1)


def main_kernel(row_count, col_count, loads, *refs):
    (
        cells_hbm,
        residual_hbm,
        restriction_hbm,
        present_hbm,
        inverse_hbm,
        blocks_hbm,
        pattern_hbm,
        values_hbm,
        last_hbm,
        planes_hbm,
    ) = refs[:10]
    slots = refs[10 : 10 + SLOT_REFS]
    (
        places,
        cells,
        slots_all,
        places_all,
        total,
        digits,
        residual,
        restriction,
        present_all,
        inverse_ref,
        blocks_ref,
        pattern_ref,
        stage,
        sent,
        chunk,
        table,
        ordered,
        rhs,
        planes_ref,
        base,
        x,
        mixed,
        edge,
        halo,
        both,
        sides,
        ends_in,
        packed,
        arrived,
        values,
        residual_sem,
        restriction_sem,
        small_sem,
        slots_sem,
        send_sem,
        recv_sem,
        halo_send_sem,
        halo_recv_sem,
        back_send_sem,
        back_recv_sem,
        values_sem,
    ) = refs[10 + SLOT_REFS :]
    devices = row_count * col_count
    parts = LANES // devices
    pairs = residual.shape[0]
    width = residual.shape[-1]
    height = inverse_ref.shape[2]
    few = PAIR * parts
    piece = pairs * few
    row = lax.axis_index("row")
    col = lax.axis_index("col")
    me = row * col_count + col
    rows = 3 * few
    half_width = width // PAIR
    small = [
        pltpu.make_async_copy(present_hbm, present_all, small_sem.at[0]),
        pltpu.make_async_copy(cells_hbm, cells, small_sem.at[1]),
        pltpu.make_async_copy(inverse_hbm, inverse_ref, small_sem.at[2]),
        pltpu.make_async_copy(blocks_hbm, blocks_ref, small_sem.at[3]),
        pltpu.make_async_copy(pattern_hbm, pattern_ref, small_sem.at[4]),
    ]

    def load(pair, first_lane, count, which):
        for p in range(FPA):
            lanes = pl.ds((p * pairs + pair) * width + first_lane, count)
            target = residual.at[pair, p, :, :, pl.ds(first_lane, count)]
            pltpu.make_async_copy(residual_hbm.at[:, :, lanes], target, residual_sem.at[which]).start()
            target = restriction.at[:, :, lanes]
            pltpu.make_async_copy(restriction_hbm.at[:, :, lanes], target, restriction_sem.at[which]).start()

    def loaded(pair, first_lane, count, which):
        target = residual.at[pair, :, :, :, pl.ds(first_lane, count)]
        pltpu.make_async_copy(target, target, residual_sem.at[which]).wait()
        target = restriction.at[:, :, pl.ds(0, FPA * count)]
        pltpu.make_async_copy(target, target, restriction_sem.at[which]).wait()

    small[0].start()
    load(0, 0, half_width, 0)
    barrier = greet(devices, col_count, me)
    load(0, half_width, half_width, pairs)
    halo[...] = jnp.zeros_like(halo)
    edge[...] = jnp.zeros_like(edge)
    ends_in[...] = jnp.zeros_like(ends_in)
    both[...] = jnp.zeros_like(both)
    small[0].wait()

    near = devices // 2

    def send_first(pair):
        def send(index, carry):
            peer, where = peer_of(me, index, devices, col_count)
            pltpu.make_async_remote_copy(
                src_ref=sent.at[pl.ds((pair * devices + peer) * rows, rows)],
                dst_ref=chunk.at[pair, me],
                send_sem=send_sem,
                recv_sem=recv_sem.at[pair, index // near],
                device_id=where,
                device_id_type=MESH,
            ).start()
            return carry

        lax.fori_loop(1, devices, send, 0)

    def restrict(pair, split):
        if not split:
            loaded(pair, 0, width, pair)
        for half in range(PAIR):
            if split:
                loaded(pair, half * half_width, half_width, pairs if half else 0)
            for block in range(GROUP):
                start = (half * GROUP + block) * LANES
                lanes = slice(start, start + LANES)
                which = half * GROUP + block
                totals = [None, None, None]
                for p in range(FPA):
                    there = pl.ds(pl.multiple_of((p * pairs + pair) * width + start, LANES), LANES)
                    present = present_all[p * pairs + pair, which : which + 1, :].astype(jnp.float32)
                    for j in range(3):
                        masked = residual[pair, p, j, :, lanes] * present
                        for i in range(3):
                            term = restriction[i, j : j + 1, there] * masked
                            totals[i] = term if totals[i] is None else totals[i] + term
                for i in range(3):
                    stage[i, block * loads : (block + 1) * loads, :] = totals[i]
            for i in range(3):
                turned = stage[i].T
                for part in range(parts):
                    at = pair * (devices * rows) + (i * PAIR + half) * parts + part
                    sent[pl.ds(at, devices, stride=rows), :] = turned[part * devices : (part + 1) * devices, :]

    restrict(0, True)
    pl.semaphore_wait(barrier, devices - 1)
    send_first(0)
    for pair in range(1, pairs):
        load(pair, 0, width, pair)
    for copy in small[1:]:
        copy.start()

    def later(pair, carry):
        restrict(pair, False)
        send_first(pair)
        return carry

    lax.fori_loop(1, pairs, later, 0)
    for copy in small[1:]:
        copy.wait()

    def keep(pair, carry):
        chunk[pair, me] = sent[pl.ds((pair * devices + me) * rows, rows), :]
        return carry

    lax.fori_loop(0, pairs, keep, 0)

    def fold(d, carry):
        on = pattern_ref[d].astype(jnp.float32)
        for k in range(3):
            column = [blocks_ref[d, j, k] * on for j in range(3)]
            for i in range(3):
                total = inverse_ref[i, 0] * column[0]
                total = total + inverse_ref[i, 1] * column[1]
                mixed[d, i, k] = total + inverse_ref[i, 2] * column[2]
        return carry

    lax.fori_loop(0, 4, fold, 0)
    fill_tables(devices, cells, slots_all, places_all, total, digits)
    lines = slots[0].shape[0]
    moves = [pltpu.make_async_copy(places_all, places, small_sem.at[0])]
    for n in range(SLOT_REFS):
        moves.append(pltpu.make_async_copy(slots_all.at[pl.ds(n * lines, lines)], slots[n], slots_sem.at[n]))
    for move in moves:
        move.start()
    for move in moves:
        move.wait()
    _, where = peer_of(me, 1, devices, col_count)

    def first_exchange(pair, messages, group):
        return pltpu.make_async_remote_copy(
            src_ref=chunk.at[pair, pl.ds(0, messages)],
            dst_ref=chunk.at[pair, pl.ds(0, messages)],
            send_sem=send_sem,
            recv_sem=recv_sem.at[pair, group],
            device_id=where,
            device_id_type=MESH,
        )

    def aligned(at):
        return pl.multiple_of(at, few) if few % 8 == 0 else at

    lane_few = lax.broadcasted_iota(jnp.int32, (few, LANES), 1) // loads

    def unpack(pair, carry):
        for group in range(2):
            first_exchange(pair, near - 1 if group == 0 else near, group).wait_recv()

            def some(step, carry):
                for n in range(BATCH):
                    f = lax.rem(me + devices - (group * near + step * BATCH + n), devices)
                    parts_i = [chunk[pair, f, i * few : (i + 1) * few, :] for i in range(3)]
                    moved = [parts_i[0], pltpu.roll(parts_i[1], loads, 1), pltpu.roll(parts_i[2], 2 * loads, 1)]
                    for some_blocks in ((0, 3), (1, 4), (2, 5), (6,), (7,)):
                        second = functools.reduce(jnp.logical_or, [lane_few == (b + 1) % GROUP for b in some_blocks])
                        third = functools.reduce(jnp.logical_or, [lane_few == (b + 2) % GROUP for b in some_blocks])
                        mix = jnp.where(third, moved[2], jnp.where(second, moved[1], moved[0]))
                        for b in some_blocks:
                            line = pltpu.roll(mix, (LANES - b * loads) % LANES, 1) if b else mix
                            at = aligned(f * (GROUP * piece) + b * piece + pair * few)
                            table[pl.ds(at, few), :] = line
                return carry

            lax.fori_loop(0, near // BATCH, some, 0)
        return carry

    lax.fori_loop(0, pairs, unpack, 0)
    sent_all = pltpu.make_async_remote_copy(
        src_ref=chunk.at[:, pl.ds(0, devices - 1)],
        dst_ref=chunk.at[:, pl.ds(0, devices - 1)],
        send_sem=send_sem,
        recv_sem=recv_sem.at[0, 0],
        device_id=where,
        device_id_type=MESH,
    )
    sent_all.wait_send()

    span = lines * LANES

    def take(line, carry):
        for j in range(LANES):
            for n in range(SLOT_REFS):
                ordered[pl.ds(n * span + line * LANES + j, 1), :] = table[pl.ds(slots[n][line, j], 1), :]
        return carry

    lax.fori_loop(0, lines, take, 0)

    def turn(r, carry):
        turned = ordered[pl.ds(pl.multiple_of(r * LANES, LANES), LANES), :].T
        rhs[pl.ds(r, 3 * loads, stride=height), :] = turned[: 3 * loads, :]
        return carry

    lax.fori_loop(0, height, turn, 0, unroll=24)

    part_loads = loads // HALVES
    planes = 3 * part_loads
    end_rows = ends_in.shape[1]
    exists = (row > 0, row < row_count - 1, col > 0, col < col_count - 1)
    peers = (
        {"row": row - 1, "col": col},
        {"row": row + 1, "col": col},
        {"row": row, "col": col - 1},
        {"row": row, "col": col + 1},
    )
    lane = lax.broadcasted_iota(jnp.int32, (height, LANES), 1)

    def plane_rows(index):
        return pl.ds(pl.multiple_of(index * height, height), height)

    def first(half):
        def one(q, carry):
            source = half * part_loads + q
            given = [rhs[plane_rows(j * loads + source), :] for j in range(3)]
            for i in range(3):
                total = inverse_ref[i, 0] * given[0]
                total = total + inverse_ref[i, 1] * given[1]
                total = total + inverse_ref[i, 2] * given[2]
                base[half * planes + i * part_loads + q] = total
                x[0, half * planes + i * part_loads + q, 8 : 8 + height, :] = total
            return carry

        lax.fori_loop(0, part_loads, one, 0, unroll=4)

    def pack(slot, step, half):
        own = slice(half * planes, (half + 1) * planes)
        edge[step, half, 0] = x[slot, own, 8, :]
        edge[step, half, 1] = x[slot, own, 7 + height, :]

        def columns(p, mix):
            moved = pltpu.roll(x[slot, half * planes + p, 8 : 8 + height, :], 2 * p + 1, 1)
            return jnp.where(lane // 2 == p, moved, mix)

        mix = lax.fori_loop(0, planes, columns, jnp.zeros((height, LANES), jnp.float32), unroll=12)
        sides[half, : 2 * planes, :height] = mix.T[: 2 * planes]
        edge[step, half, 2, :, :height] = sides[half, pl.ds(1, planes, stride=2), :height]
        edge[step, half, 3, :, :height] = sides[half, pl.ds(0, planes, stride=2), :height]

    def copy_edge(step, half, d, side):
        return pltpu.make_async_remote_copy(
            src_ref=edge.at[step, half, d],
            dst_ref=halo.at[step, half, side],
            send_sem=halo_send_sem.at[step, half, d],
            recv_sem=halo_recv_sem.at[step, half, side],
            device_id=peers[d],
            device_id_type=MESH,
        )

    def start(step, half):
        for d in range(4):

            @pl.when(exists[d])
            def _():
                copy_edge(step, half, d, d ^ 1).start()

    for half in range(HALVES):
        first(half)
        pack(0, 0, half)
        start(0, half)
    for step in range(ITERS - 1):
        old = step % 2
        last = step == ITERS - 2
        for half in range(HALVES):
            for d in range(4):

                @pl.when(exists[d])
                def _():
                    copy_edge(step, half, d, d).wait_send()
                    copy_edge(step, half, d, d).wait_recv()

            own = slice(half * planes, (half + 1) * planes)
            x[old, own, 7, :] = halo[step, half, 0]
            x[old, own, 8 + height, :] = halo[step, half, 1]
            ends_in[half, pl.ds(2, planes, stride=2), :] = halo[step, half, 2]
            ends_in[half, pl.ds(1, planes, stride=2), :] = halo[step, half, 3]
            both[half, :, :end_rows] = ends_in[half].T[:height]

            def update(q, carry):
                totals = [base[half * planes + i * part_loads + q] for i in range(3)]
                for k in range(3):
                    local = k * part_loads + q
                    p = half * planes + local
                    plane = x[old, p, 8 : 8 + height, :]
                    ends = pltpu.roll(both[half], LANES - 2 - 2 * local, 1)
                    left = jnp.where(lane == 0, ends, pltpu.roll(plane, 1, 1))
                    right = jnp.where(lane == LANES - 1, ends, pltpu.roll(plane, LANES - 1, 1))
                    shifted = (x[old, p, 7 : 7 + height, :], x[old, p, 9 : 9 + height, :], left, right)
                    for d in range(4):
                        for i in range(3):
                            totals[i] = totals[i] - mixed[d, i, k] * shifted[d]
                for i in range(3):
                    if last:
                        planes_ref[plane_rows(i * loads + half * part_loads + q), :] = totals[i]
                    else:
                        x[1 - old, half * planes + i * part_loads + q, 8 : 8 + height, :] = totals[i]
                return carry

            lax.fori_loop(0, part_loads, update, 0, unroll=4)
            if not last:
                pack(1 - old, step + 1, half)
                start(step + 1, half)

    out_copy = pltpu.make_async_copy(planes_ref, planes_hbm, small_sem.at[0])
    out_copy.start()

    def back(r, carry):
        plane = planes_ref[pl.ds(r, 3 * loads, stride=height), :]
        ordered[pl.ds(pl.multiple_of(r * LANES, LANES), LANES), : 3 * loads] = plane.T
        return carry

    lax.fori_loop(0, height, back, 0, unroll=24)
    lane_few = lax.broadcasted_iota(jnp.int32, (few, LANES), 1)

    def pack_back(pair, peer, at):
        for block in range(GROUP):
            for n in range(few):
                line = (pair * PAIR + n // parts) * GROUP + block
                source = places[line, (n % parts) * devices + peer]
                table[pl.ds(at + block * few + n, 1), :] = ordered[pl.ds(source, 1), :]
        lines = [table[at + block * few : at + (block + 1) * few, :] for block in range(GROUP)]
        results = []
        for i in range(3):
            result = None
            for block in range(GROUP):
                shift = ((block - i) * loads) % LANES
                moved = pltpu.roll(lines[block], shift, 1) if shift else lines[block]
                result = moved if result is None else jnp.where(lane_few < block * loads, result, moved)
            results.append(result)
        return results

    def place_of(pair, device):
        return (pair * devices + device) * rows

    def give_back(pair, final):
        def give(step, carry):
            for n in range(2):
                index = 2 * step + 1 + n
                peer, where = peer_of(me, index, devices, col_count)
                results = pack_back(pair, peer, n * GROUP * few)
                for i in range(3):
                    packed[pl.ds(place_of(pair, peer) + i * few, few), :] = results[i]

                def send():
                    target = last_hbm.at[me] if final else arrived.at[pl.ds(place_of(pair, me), rows)]
                    pltpu.make_async_remote_copy(
                        src_ref=packed.at[pl.ds(place_of(pair, peer), rows)],
                        dst_ref=target,
                        send_sem=back_send_sem.at[pair],
                        recv_sem=back_recv_sem.at[pair],
                        device_id=where,
                        device_id_type=MESH,
                    ).start()

                if n == 0:
                    send()
                else:
                    pl.when(index < devices)(send)
            return carry

        lax.fori_loop(0, devices // 2, give, 0)
        if not final:
            arrived[pl.ds(place_of(pair, me), rows), :] = packed[pl.ds(place_of(pair, me), rows), :]

    def give_early(pair, carry):
        give_back(pair, False)
        return carry

    final = pairs - 1
    lax.fori_loop(0, final, give_early, 0)
    give_back(final, True)
    own = pltpu.make_async_copy(packed.at[pl.ds(place_of(final, me), rows)], last_hbm.at[me], values_sem.at[final])
    own.start()
    for pair in range(final):
        _, where = peer_of(me, 1, devices, col_count)
        every = pltpu.make_async_remote_copy(
            src_ref=packed.at[pl.ds(place_of(pair, 0), (devices - 1) * rows)],
            dst_ref=arrived.at[pl.ds(place_of(pair, 0), (devices - 1) * rows)],
            send_sem=back_send_sem.at[pair],
            recv_sem=back_recv_sem.at[pair],
            device_id=where,
            device_id_type=MESH,
        )
        every.wait_send()
        every.wait_recv()
        for i in range(3):
            for half in range(PAIR):
                at = place_of(pair, 0) + (i * PAIR + half) * parts
                pieces = [arrived[pl.ds(at + part, devices, stride=rows), :] for part in range(parts)]
                values[pair, i, half] = jnp.concatenate(pieces, axis=0).T if parts > 1 else pieces[0].T
        pltpu.make_async_copy(values.at[pair], values_hbm.at[pair], values_sem.at[pair]).start()
    out_copy.wait()
    own.wait()
    for pair in range(final):
        pltpu.make_async_copy(values.at[pair], values_hbm.at[pair], values_sem.at[pair]).wait()
    _, where = peer_of(me, 1, devices, col_count)
    every = pltpu.make_async_remote_copy(
        src_ref=last_hbm.at[pl.ds(0, devices - 1)],
        dst_ref=last_hbm.at[pl.ds(0, devices - 1)],
        send_sem=back_send_sem.at[final],
        recv_sem=back_recv_sem.at[final],
        device_id=where,
        device_id_type=MESH,
    )
    every.wait_send()
    every.wait_recv()


def main(cells, residual, restriction, present, inverse, blocks, pattern, row_count, col_count):
    loads = residual.shape[0]
    residual = residual.transpose(1, 0, 2)
    devices = row_count * col_count
    parts = LANES // devices
    width = LANES * GROUP * PAIR
    pairs = AGG_DEV // width
    present = present.reshape(-1, GROUP * PAIR, LANES)
    height = inverse.shape[2]
    rows = 3 * PAIR * parts
    planes = 3 * loads
    steps = ITERS - 1
    part_planes = planes // HALVES
    end_rows = -(-(2 * part_planes + 2) // 8) * 8
    count = height * LANES
    blocks_own = AGG_DEV // LANES
    dma = pltpu.SemaphoreType.DMA
    scratch = [pltpu.SMEM((height // SLOT_REFS, LANES), jnp.int32) for _ in range(SLOT_REFS)]
    scratch += [
        pltpu.SMEM((blocks_own, LANES), jnp.int32),
        pltpu.VMEM((height, LANES), jnp.int32),
        pltpu.VMEM((height, LANES), jnp.int32),
        pltpu.VMEM((blocks_own, LANES), jnp.int32),
        pltpu.VMEM((2 * blocks_own, LANES), jnp.float32),
        pltpu.VMEM((2, height, LANES), jnp.float32),
        pltpu.VMEM((pairs, FPA, 3, loads, width), jnp.float32),
        pltpu.VMEM(restriction.shape, jnp.float32),
        pltpu.VMEM(present.shape, jnp.int32),
        pltpu.VMEM(inverse.shape, jnp.float32),
        pltpu.VMEM(blocks.shape, jnp.float32),
        pltpu.VMEM(pattern.shape, jnp.int32),
        pltpu.VMEM((3, LANES, LANES), jnp.float32),
        pltpu.VMEM((pairs * devices * rows, LANES), jnp.float32),
        pltpu.VMEM((pairs, devices, rows, LANES), jnp.float32),
        pltpu.VMEM((AGG_DEV, LANES), jnp.float32),
        pltpu.VMEM((count, LANES), jnp.float32),
        pltpu.VMEM((planes * height, LANES), jnp.float32),
        pltpu.VMEM((planes * height, LANES), jnp.float32),
        pltpu.VMEM((planes, height, LANES), jnp.float32),
        pltpu.VMEM((2, planes, height + 16, LANES), jnp.float32),
        pltpu.VMEM((4, 3, 3, height, LANES), jnp.float32),
        pltpu.VMEM((steps, HALVES, 4, part_planes, LANES), jnp.float32),
        pltpu.VMEM((steps, HALVES, 4, part_planes, LANES), jnp.float32),
        pltpu.VMEM((HALVES, height, LANES), jnp.float32),
        pltpu.VMEM((HALVES, end_rows, LANES), jnp.float32),
        pltpu.VMEM((HALVES, end_rows, LANES), jnp.float32),
        pltpu.VMEM((pairs * devices * rows, LANES), jnp.float32),
        pltpu.VMEM(((pairs - 1) * devices * rows, LANES), jnp.float32),
        pltpu.VMEM((pairs - 1, 3, PAIR, LANES, LANES), jnp.float32),
        dma((pairs + 1,)),
        dma((pairs + 1,)),
        dma((5,)),
        dma((SLOT_REFS,)),
        dma,
        dma((pairs, 2)),
        dma((steps, HALVES, 4)),
        dma((steps, HALVES, 4)),
        dma((pairs,)),
        dma((pairs,)),
        dma((pairs,)),
    ]
    return pl.pallas_call(
        functools.partial(main_kernel, row_count, col_count, loads),
        in_specs=[spec_any()] * 7,
        out_specs=(spec_any(), spec_any(), spec_any()),
        out_shape=(
            jax.ShapeDtypeStruct((pairs - 1, 3, PAIR, LANES, LANES), jnp.float32),
            jax.ShapeDtypeStruct((devices, rows, LANES), jnp.float32),
            jax.ShapeDtypeStruct((planes * height, LANES), jnp.float32),
        ),
        scratch_shapes=scratch,
        compiler_params=pltpu.CompilerParams(vmem_limit_bytes=VMEM_LIMIT, collective_id=1, has_side_effects=True),
        name="correct",
    )(cells, residual, restriction, present, inverse, blocks, pattern)


def prolong_kernel(
    devices,
    values_hbm,
    last_hbm,
    restriction_hbm,
    pattern_hbm,
    planes_hbm,
    out_hbm,
    iterate_hbm,
    values,
    last,
    restriction,
    pattern,
    planes,
    out,
    restriction_sem,
    small_sem,
    out_sem,
    iterate_sem,
):
    final = values.shape[0] - 1
    parts = LANES // devices
    rows = last.shape[0] // devices
    loads = out.shape[1]
    blocks = AGG_DEV // LANES

    def slab(p):
        return pl.ds(pl.multiple_of(p * AGG_DEV, LANES), AGG_DEV)

    def restriction_copy(p):
        return pltpu.make_async_copy(restriction_hbm.at[:, :, slab(p)], restriction.at[:, :, slab(p)], restriction_sem.at[p])

    def out_copy(p):
        return pltpu.make_async_copy(out.at[:, :, slab(p)], out_hbm.at[:, :, slab(p)], out_sem.at[p])

    small = [
        pltpu.make_async_copy(pattern_hbm, pattern, small_sem.at[0]),
        pltpu.make_async_copy(values_hbm, values.at[pl.ds(0, final)], small_sem.at[1]),
        pltpu.make_async_copy(last_hbm, last, small_sem.at[3]),
        pltpu.make_async_copy(planes_hbm, planes, small_sem.at[2]),
    ]
    small[2].start()
    small[1].start()
    small[0].start()
    for p in range(FPA):
        restriction_copy(p).start()
    small[3].start()
    small[2].wait()
    for i in range(3):
        for half in range(PAIR):
            at = (i * PAIR + half) * parts
            pieces = [last[pl.ds(at + part, devices, stride=rows), :] for part in range(parts)]
            values[final, i, half] = jnp.concatenate(pieces, axis=0).T if parts > 1 else pieces[0].T
    small[0].wait()
    small[1].wait()

    def one(p, carry):
        restriction_copy(p).wait()
        for b in range(blocks):
            pair, half, block = b // (GROUP * PAIR), b // GROUP % PAIR, b % GROUP
            lanes = pl.ds(pl.multiple_of(p * AGG_DEV + b * LANES, LANES), LANES)
            present = pattern[pl.ds(p * blocks + b, 1), :].astype(jnp.float32)
            terms = [values[pair, i, half, block * loads : (block + 1) * loads, :] * present for i in range(3)]
            for j in range(3):
                total = restriction[0, j : j + 1, lanes] * terms[0]
                total = total + restriction[1, j : j + 1, lanes] * terms[1]
                out[j, :, lanes] = total + restriction[2, j : j + 1, lanes] * terms[2]
        out_copy(p).start()
        return carry

    lax.fori_loop(0, FPA, one, 0)
    small[3].wait()
    turned = [pltpu.make_async_copy(planes.at[i], iterate_hbm.at[:, i], iterate_sem.at[i]) for i in range(3)]
    for copy in turned:
        copy.start()
    for copy in turned:
        copy.wait()
    for p in range(FPA):
        out_copy(p).wait()


def prolong(values, last, restriction, pattern, planes, loads, height):
    pattern = pattern.reshape(-1, LANES)
    planes = planes.reshape(3, loads, height, LANES)
    devices = last.shape[0]
    last = last.reshape(-1, LANES)
    dma = pltpu.SemaphoreType.DMA
    shape = (3, loads, restriction.shape[2])
    out, iterate = pl.pallas_call(
        functools.partial(prolong_kernel, devices),
        in_specs=[spec_any()] * 5,
        out_specs=(spec_any(), spec_any()),
        out_shape=(
            jax.ShapeDtypeStruct(shape, jnp.float32),
            jax.ShapeDtypeStruct((loads, 3, height, LANES), jnp.float32),
        ),
        scratch_shapes=[
            pltpu.VMEM((values.shape[0] + 1,) + values.shape[1:], jnp.float32),
            pltpu.VMEM(last.shape, jnp.float32),
            pltpu.VMEM(restriction.shape, jnp.float32),
            pltpu.VMEM(pattern.shape, jnp.int32),
            pltpu.VMEM(planes.shape, jnp.float32),
            pltpu.VMEM(shape, jnp.float32),
            dma((FPA,)),
            dma((4,)),
            dma((FPA,)),
            dma((3,)),
        ],
        compiler_params=pltpu.CompilerParams(vmem_limit_bytes=VMEM_LIMIT),
        name="prolong",
    )(values, last, restriction, pattern, planes)
    return out.transpose(1, 0, 2), iterate


def body(
    fine_residual,
    restriction,
    restriction_pattern,
    cell_aggregate,
    block_inverse,
    off_blocks,
    operator_pattern,
):
    loads = fine_residual.shape[0]
    row_count = lax.axis_size("row")
    col_count = lax.axis_size("col")
    height = cell_aggregate.shape[0]
    values, last, planes = main(
        cell_aggregate,
        fine_residual,
        restriction,
        restriction_pattern,
        block_inverse,
        off_blocks,
        operator_pattern,
        row_count,
        col_count,
    )
    fine_correction, iterate = prolong(values, last, restriction, restriction_pattern, planes, loads, height)
    return (iterate, fine_correction)


def solution(mesh):
    in_specs = (
        P(None, None, ("row", "col")),
        P(None, None, ("row", "col")),
        P(("row", "col")),
        P("row", "col"),
        P(None, None, "row", "col"),
        P(None, None, None, "row", "col"),
        P(None, "row", "col"),
    )
    out_specs = (P(None, None, "row", "col"), P(None, None, ("row", "col")))
    return jax.shard_map(body, mesh=mesh, in_specs=in_specs, out_specs=out_specs, check_vma=False)
```

```python
import functools

import jax
import jax.numpy as jnp
from jax import lax
from jax.experimental import pallas as pl
from jax.experimental.pallas import tpu as pltpu
from jax.sharding import PartitionSpec as P

FPA = 8
ITERS = 4
AGG_DEV = 6144
LANES = 128
GROUP = 8
PAIR = 2
HALVES = 4
BATCH = 16
SLOT_REFS = 6
MESH = pl.DeviceIdType.MESH
VMEM_LIMIT = 56 * 1024 * 1024


def spec_vmem():
    return pl.BlockSpec(memory_space=pltpu.VMEM)


def spec_any():
    return pl.BlockSpec(memory_space=pl.ANY)


def peer_of(me, index, devices, col_count):
    peer = lax.rem(me + index, devices)
    return peer, {"row": lax.div(peer, col_count), "col": lax.rem(peer, col_count)}


def greet(devices, col_count, me):
    barrier = pltpu.get_barrier_semaphore()

    def signal(index, carry):
        _, where = peer_of(me, index, devices, col_count)
        pl.semaphore_signal(barrier, inc=1, device_id=where, device_id_type=MESH)
        return carry

    lax.fori_loop(1, devices, signal, 0)
    return barrier


def fill_tables(devices, cells_ref, slots_ref, inverse_ref, total_ref, owner_ref):
    height = cells_ref.shape[0]
    parts = LANES // devices
    blocks = AGG_DEV // LANES
    piece = blocks * parts // GROUP
    value = cells_ref[...].astype(jnp.float32)
    owner = jnp.floor((value + 0.5) * (1.0 / AGG_DEV))
    inside = value - owner * AGG_DEV
    block = jnp.floor((inside + 0.5) * (1.0 / LANES))
    part = jnp.floor((inside - block * LANES + 0.5) * (1.0 / devices))
    group = jnp.floor((block + 0.5) * (1.0 / GROUP))
    slot = owner * (GROUP * piece) + (block - group * GROUP) * piece + group * parts + part
    slots_ref[...] = jnp.clip(slot.astype(jnp.int32), 0, AGG_DEV - 1)
    owner_ref[0] = block
    owner_ref[1] = part * devices + owner
    rows = lax.broadcasted_iota(jnp.int32, (blocks, LANES), 0).astype(jnp.float32)
    lanes = lax.broadcasted_iota(jnp.int32, (blocks, LANES), 1).astype(jnp.float32)
    places = lax.broadcasted_iota(jnp.int32, (LANES, LANES), 0).astype(jnp.float32)
    total_ref[...] = jnp.zeros_like(total_ref)

    def some(r, carry):
        hit = rows == owner_ref[0, pl.ds(r, 1), :]
        low = jnp.where(hit, lanes, 0.0)
        high = jnp.where(hit, r.astype(jnp.float32), 0.0)
        left = jnp.concatenate([low, high], axis=0).astype(jnp.bfloat16)
        right = jnp.where(places == owner_ref[1, pl.ds(r, 1), :], 1.0, 0.0).astype(jnp.bfloat16)
        total_ref[...] += lax.dot_general(left, right, (((1,), (1,)), ((), ())), preferred_element_type=jnp.float32)
        return carry

    lax.fori_loop(0, height, some, 0, unroll=4)
    inverse = (total_ref[:blocks] + total_ref[blocks:] * LANES).astype(jnp.int32)
    inverse_ref[...] = jnp.clip(inverse, 0, height * LANES - 1)


def main_kernel(row_count, col_count, loads, *refs):
    (
        cells_hbm,
        residual_hbm,
        restriction_hbm,
        present_hbm,
        inverse_hbm,
        blocks_hbm,
        pattern_hbm,
        values_hbm,
        last_hbm,
        planes_hbm,
    ) = refs[:10]
    slots = refs[10 : 10 + SLOT_REFS]
    (
        places,
        cells,
        slots_all,
        places_all,
        total,
        digits,
        residual,
        restriction,
        present_all,
        inverse_ref,
        blocks_ref,
        pattern_ref,
        stage,
        sent,
        chunk,
        table,
        ordered,
        rhs,
        planes_ref,
        base,
        x,
        mixed,
        edge,
        halo,
        both,
        sides,
        ends_in,
        packed,
        arrived,
        values,
        residual_sem,
        restriction_sem,
        small_sem,
        slots_sem,
        send_sem,
        recv_sem,
        halo_send_sem,
        halo_recv_sem,
        back_send_sem,
        back_recv_sem,
        values_sem,
    ) = refs[10 + SLOT_REFS :]
    devices = row_count * col_count
    parts = LANES // devices
    pairs = residual.shape[0]
    width = residual.shape[-1]
    height = inverse_ref.shape[2]
    few = PAIR * parts
    piece = pairs * few
    row = lax.axis_index("row")
    col = lax.axis_index("col")
    me = row * col_count + col
    rows = 3 * few
    half_width = width // PAIR
    small = [
        pltpu.make_async_copy(present_hbm, present_all, small_sem.at[0]),
        pltpu.make_async_copy(cells_hbm, cells, small_sem.at[1]),
        pltpu.make_async_copy(inverse_hbm, inverse_ref, small_sem.at[2]),
        pltpu.make_async_copy(blocks_hbm, blocks_ref, small_sem.at[3]),
        pltpu.make_async_copy(pattern_hbm, pattern_ref, small_sem.at[4]),
    ]

    def load(pair, first_lane, count, which):
        for p in range(FPA):
            lanes = pl.ds((p * pairs + pair) * width + first_lane, count)
            target = residual.at[pair, p, :, :, pl.ds(first_lane, count)]
            pltpu.make_async_copy(residual_hbm.at[:, :, lanes], target, residual_sem.at[which]).start()
            target = restriction.at[:, :, lanes]
            pltpu.make_async_copy(restriction_hbm.at[:, :, lanes], target, restriction_sem.at[which]).start()

    def loaded(pair, first_lane, count, which):
        target = residual.at[pair, :, :, :, pl.ds(first_lane, count)]
        pltpu.make_async_copy(target, target, residual_sem.at[which]).wait()
        target = restriction.at[:, :, pl.ds(0, FPA * count)]
        pltpu.make_async_copy(target, target, restriction_sem.at[which]).wait()

    small[0].start()
    load(0, 0, half_width, 0)
    barrier = greet(devices, col_count, me)
    load(0, half_width, half_width, pairs)
    halo[...] = jnp.zeros_like(halo)
    edge[...] = jnp.zeros_like(edge)
    ends_in[...] = jnp.zeros_like(ends_in)
    both[...] = jnp.zeros_like(both)
    small[0].wait()

    near = devices // 2

    def send_first(pair):
        def send(index, carry):
            peer, where = peer_of(me, index, devices, col_count)
            pltpu.make_async_remote_copy(
                src_ref=sent.at[pl.ds((pair * devices + peer) * rows, rows)],
                dst_ref=chunk.at[pair, me],
                send_sem=send_sem,
                recv_sem=recv_sem.at[pair, index // near],
                device_id=where,
                device_id_type=MESH,
            ).start()
            return carry

        lax.fori_loop(1, devices, send, 0)

    def restrict(pair, split):
        if not split:
            loaded(pair, 0, width, pair)
        for half in range(PAIR):
            if split:
                loaded(pair, half * half_width, half_width, pairs if half else 0)
            for block in range(GROUP):
                start = (half * GROUP + block) * LANES
                lanes = slice(start, start + LANES)
                which = half * GROUP + block
                totals = [None, None, None]
                for p in range(FPA):
                    there = pl.ds(pl.multiple_of((p * pairs + pair) * width + start, LANES), LANES)
                    present = present_all[p * pairs + pair, which : which + 1, :].astype(jnp.float32)
                    for j in range(3):
                        masked = residual[pair, p, j, :, lanes] * present
                        for i in range(3):
                            term = restriction[i, j : j + 1, there] * masked
                            totals[i] = term if totals[i] is None else totals[i] + term
                for i in range(3):
                    stage[i, block * loads : (block + 1) * loads, :] = totals[i]
            for i in range(3):
                turned = stage[i].T
                for part in range(parts):
                    at = pair * (devices * rows) + (i * PAIR + half) * parts + part
                    sent[pl.ds(at, devices, stride=rows), :] = turned[part * devices : (part + 1) * devices, :]

    restrict(0, True)
    pl.semaphore_wait(barrier, devices - 1)
    send_first(0)
    for pair in range(1, pairs):
        load(pair, 0, width, pair)
    for copy in small[1:]:
        copy.start()

    def later(pair, carry):
        restrict(pair, False)
        send_first(pair)
        return carry

    lax.fori_loop(1, pairs, later, 0)
    for copy in small[1:]:
        copy.wait()

    def keep(pair, carry):
        chunk[pair, me] = sent[pl.ds((pair * devices + me) * rows, rows), :]
        return carry

    lax.fori_loop(0, pairs, keep, 0)

    def fold(d, carry):
        on = pattern_ref[d].astype(jnp.float32)
        for k in range(3):
            column = [blocks_ref[d, j, k] * on for j in range(3)]
            for i in range(3):
                total = inverse_ref[i, 0] * column[0]
                total = total + inverse_ref[i, 1] * column[1]
                mixed[d, i, k] = total + inverse_ref[i, 2] * column[2]
        return carry

    lax.fori_loop(0, 4, fold, 0)
    fill_tables(devices, cells, slots_all, places_all, total, digits)
    lines = slots[0].shape[0]
    moves = [pltpu.make_async_copy(places_all, places, small_sem.at[0])]
    for n in range(SLOT_REFS):
        moves.append(pltpu.make_async_copy(slots_all.at[pl.ds(n * lines, lines)], slots[n], slots_sem.at[n]))
    for move in moves:
        move.start()
    for move in moves:
        move.wait()
    _, where = peer_of(me, 1, devices, col_count)

    def first_exchange(pair, messages, group):
        return pltpu.make_async_remote_copy(
            src_ref=chunk.at[pair, pl.ds(0, messages)],
            dst_ref=chunk.at[pair, pl.ds(0, messages)],
            send_sem=send_sem,
            recv_sem=recv_sem.at[pair, group],
            device_id=where,
            device_id_type=MESH,
        )

    def aligned(at):
        return pl.multiple_of(at, few) if few % 8 == 0 else at

    lane_few = lax.broadcasted_iota(jnp.int32, (few, LANES), 1) // loads

    def unpack(pair, carry):
        for group in range(2):
            first_exchange(pair, near - 1 if group == 0 else near, group).wait_recv()

            def some(step, carry):
                for n in range(BATCH):
                    f = lax.rem(me + devices - (group * near + step * BATCH + n), devices)
                    parts_i = [chunk[pair, f, i * few : (i + 1) * few, :] for i in range(3)]
                    moved = [parts_i[0], pltpu.roll(parts_i[1], loads, 1), pltpu.roll(parts_i[2], 2 * loads, 1)]
                    for some_blocks in ((0, 3), (1, 4), (2, 5), (6,), (7,)):
                        second = functools.reduce(jnp.logical_or, [lane_few == (b + 1) % GROUP for b in some_blocks])
                        third = functools.reduce(jnp.logical_or, [lane_few == (b + 2) % GROUP for b in some_blocks])
                        mix = jnp.where(third, moved[2], jnp.where(second, moved[1], moved[0]))
                        for b in some_blocks:
                            line = pltpu.roll(mix, (LANES - b * loads) % LANES, 1) if b else mix
                            at = aligned(f * (GROUP * piece) + b * piece + pair * few)
                            table[pl.ds(at, few), :] = line
                return carry

            lax.fori_loop(0, near // BATCH, some, 0)
        return carry

    lax.fori_loop(0, pairs, unpack, 0)
    sent_all = pltpu.make_async_remote_copy(
        src_ref=chunk.at[:, pl.ds(0, devices - 1)],
        dst_ref=chunk.at[:, pl.ds(0, devices - 1)],
        send_sem=send_sem,
        recv_sem=recv_sem.at[0, 0],
        device_id=where,
        device_id_type=MESH,
    )
    sent_all.wait_send()

    span = lines * LANES

    def take(line, carry):
        for j in range(LANES):
            for n in range(SLOT_REFS):
                ordered[pl.ds(n * span + line * LANES + j, 1), :] = table[pl.ds(slots[n][line, j], 1), :]
        return carry

    lax.fori_loop(0, lines, take, 0)

    def turn(r, carry):
        turned = ordered[pl.ds(pl.multiple_of(r * LANES, LANES), LANES), :].T
        rhs[pl.ds(r, 3 * loads, stride=height), :] = turned[: 3 * loads, :]
        return carry

    lax.fori_loop(0, height, turn, 0, unroll=24)

    part_loads = loads // HALVES
    planes = 3 * part_loads
    end_rows = ends_in.shape[1]
    exists = (row > 0, row < row_count - 1, col > 0, col < col_count - 1)
    peers = (
        {"row": row - 1, "col": col},
        {"row": row + 1, "col": col},
        {"row": row, "col": col - 1},
        {"row": row, "col": col + 1},
    )
    lane = lax.broadcasted_iota(jnp.int32, (height, LANES), 1)

    def plane_rows(index):
        return pl.ds(pl.multiple_of(index * height, height), height)

    def first(half):
        def one(q, carry):
            source = half * part_loads + q
            given = [rhs[plane_rows(j * loads + source), :] for j in range(3)]
            for i in range(3):
                total = inverse_ref[i, 0] * given[0]
                total = total + inverse_ref[i, 1] * given[1]
                total = total + inverse_ref[i, 2] * given[2]
                base[half * planes + i * part_loads + q] = total
                x[0, half * planes + i * part_loads + q, 8 : 8 + height, :] = total
            return carry

        lax.fori_loop(0, part_loads, one, 0, unroll=4)

    def pack(slot, step, half):
        own = slice(half * planes, (half + 1) * planes)
        edge[step, half, 0] = x[slot, own, 8, :]
        edge[step, half, 1] = x[slot, own, 7 + height, :]

        def columns(p, mix):
            moved = pltpu.roll(x[slot, half * planes + p, 8 : 8 + height, :], 2 * p + 1, 1)
            return jnp.where(lane // 2 == p, moved, mix)

        mix = lax.fori_loop(0, planes, columns, jnp.zeros((height, LANES), jnp.float32), unroll=12)
        sides[half, : 2 * planes, :height] = mix.T[: 2 * planes]
        edge[step, half, 2, :, :height] = sides[half, pl.ds(1, planes, stride=2), :height]
        edge[step, half, 3, :, :height] = sides[half, pl.ds(0, planes, stride=2), :height]

    def copy_edge(step, half, d, side):
        return pltpu.make_async_remote_copy(
            src_ref=edge.at[step, half, d],
            dst_ref=halo.at[step, half, side],
            send_sem=halo_send_sem.at[step, half, d],
            recv_sem=halo_recv_sem.at[step, half, side],
            device_id=peers[d],
            device_id_type=MESH,
        )

    def start(step, half):
        for d in (2, 3, 0, 1):

            @pl.when(exists[d])
            def _():
                copy_edge(step, half, d, d ^ 1).start()

    for half in range(HALVES):
        first(half)
        pack(0, 0, half)
        start(0, half)
    for step in range(ITERS - 1):
        old = step % 2
        last = step == ITERS - 2
        for half in range(HALVES):
            for d in range(4):

                @pl.when(exists[d])
                def _():
                    copy_edge(step, half, d, d).wait_send()
                    copy_edge(step, half, d, d).wait_recv()

            own = slice(half * planes, (half + 1) * planes)
            x[old, own, 7, :] = halo[step, half, 0]
            x[old, own, 8 + height, :] = halo[step, half, 1]
            ends_in[half, pl.ds(2, planes, stride=2), :] = halo[step, half, 2]
            ends_in[half, pl.ds(1, planes, stride=2), :] = halo[step, half, 3]
            both[half, :, :end_rows] = ends_in[half].T[:height]

            def update(q, carry):
                totals = [base[half * planes + i * part_loads + q] for i in range(3)]
                for k in range(3):
                    local = k * part_loads + q
                    p = half * planes + local
                    plane = x[old, p, 8 : 8 + height, :]
                    ends = pltpu.roll(both[half], LANES - 2 - 2 * local, 1)
                    left = jnp.where(lane == 0, ends, pltpu.roll(plane, 1, 1))
                    right = jnp.where(lane == LANES - 1, ends, pltpu.roll(plane, LANES - 1, 1))
                    shifted = (x[old, p, 7 : 7 + height, :], x[old, p, 9 : 9 + height, :], left, right)
                    for d in range(4):
                        for i in range(3):
                            totals[i] = totals[i] - mixed[d, i, k] * shifted[d]
                for i in range(3):
                    if last:
                        planes_ref[plane_rows(i * loads + half * part_loads + q), :] = totals[i]
                    else:
                        x[1 - old, half * planes + i * part_loads + q, 8 : 8 + height, :] = totals[i]
                return carry

            lax.fori_loop(0, part_loads, update, 0, unroll=4)
            if not last:
                pack(1 - old, step + 1, half)
                start(step + 1, half)

    out_copy = pltpu.make_async_copy(planes_ref, planes_hbm, small_sem.at[0])
    out_copy.start()

    def back(r, carry):
        plane = planes_ref[pl.ds(r, 3 * loads, stride=height), :]
        ordered[pl.ds(pl.multiple_of(r * LANES, LANES), LANES), : 3 * loads] = plane.T
        return carry

    lax.fori_loop(0, height, back, 0, unroll=24)
    lane_few = lax.broadcasted_iota(jnp.int32, (few, LANES), 1)

    def pack_back(pair, peer, at):
        for block in range(GROUP):
            for n in range(few):
                line = (pair * PAIR + n // parts) * GROUP + block
                source = places[line, (n % parts) * devices + peer]
                table[pl.ds(at + block * few + n, 1), :] = ordered[pl.ds(source, 1), :]
        lines = [table[at + block * few : at + (block + 1) * few, :] for block in range(GROUP)]
        results = []
        for i in range(3):
            result = None
            for block in range(GROUP):
                shift = ((block - i) * loads) % LANES
                moved = pltpu.roll(lines[block], shift, 1) if shift else lines[block]
                result = moved if result is None else jnp.where(lane_few < block * loads, result, moved)
            results.append(result)
        return results

    def place_of(pair, device):
        return (pair * devices + device) * rows

    def give_back(pair, final):
        def give(step, carry):
            for n in range(2):
                index = 2 * step + 1 + n
                peer, where = peer_of(me, index, devices, col_count)
                results = pack_back(pair, peer, n * GROUP * few)
                for i in range(3):
                    packed[pl.ds(place_of(pair, peer) + i * few, few), :] = results[i]

                def send():
                    target = last_hbm.at[me] if final else arrived.at[pl.ds(place_of(pair, me), rows)]
                    pltpu.make_async_remote_copy(
                        src_ref=packed.at[pl.ds(place_of(pair, peer), rows)],
                        dst_ref=target,
                        send_sem=back_send_sem.at[pair],
                        recv_sem=back_recv_sem.at[pair],
                        device_id=where,
                        device_id_type=MESH,
                    ).start()

                if n == 0:
                    send()
                else:
                    pl.when(index < devices)(send)
            return carry

        lax.fori_loop(0, devices // 2, give, 0)
        if not final:
            arrived[pl.ds(place_of(pair, me), rows), :] = packed[pl.ds(place_of(pair, me), rows), :]

    def give_early(pair, carry):
        give_back(pair, False)
        return carry

    final = pairs - 1
    lax.fori_loop(0, final, give_early, 0)
    give_back(final, True)
    own = pltpu.make_async_copy(packed.at[pl.ds(place_of(final, me), rows)], last_hbm.at[me], values_sem.at[final])
    own.start()
    for pair in range(final):
        _, where = peer_of(me, 1, devices, col_count)
        every = pltpu.make_async_remote_copy(
            src_ref=packed.at[pl.ds(place_of(pair, 0), (devices - 1) * rows)],
            dst_ref=arrived.at[pl.ds(place_of(pair, 0), (devices - 1) * rows)],
            send_sem=back_send_sem.at[pair],
            recv_sem=back_recv_sem.at[pair],
            device_id=where,
            device_id_type=MESH,
        )
        every.wait_send()
        every.wait_recv()
        for i in range(3):
            for half in range(PAIR):
                at = place_of(pair, 0) + (i * PAIR + half) * parts
                pieces = [arrived[pl.ds(at + part, devices, stride=rows), :] for part in range(parts)]
                values[pair, i, half] = jnp.concatenate(pieces, axis=0).T if parts > 1 else pieces[0].T
        pltpu.make_async_copy(values.at[pair], values_hbm.at[pair], values_sem.at[pair]).start()
    out_copy.wait()
    own.wait()
    for pair in range(final):
        pltpu.make_async_copy(values.at[pair], values_hbm.at[pair], values_sem.at[pair]).wait()
    _, where = peer_of(me, 1, devices, col_count)
    every = pltpu.make_async_remote_copy(
        src_ref=last_hbm.at[pl.ds(0, devices - 1)],
        dst_ref=last_hbm.at[pl.ds(0, devices - 1)],
        send_sem=back_send_sem.at[final],
        recv_sem=back_recv_sem.at[final],
        device_id=where,
        device_id_type=MESH,
    )
    every.wait_send()
    every.wait_recv()


def main(cells, residual, restriction, present, inverse, blocks, pattern, row_count, col_count):
    loads = residual.shape[0]
    residual = residual.transpose(1, 0, 2)
    devices = row_count * col_count
    parts = LANES // devices
    width = LANES * GROUP * PAIR
    pairs = AGG_DEV // width
    present = present.reshape(-1, GROUP * PAIR, LANES)
    height = inverse.shape[2]
    rows = 3 * PAIR * parts
    planes = 3 * loads
    steps = ITERS - 1
    part_planes = planes // HALVES
    end_rows = -(-(2 * part_planes + 2) // 8) * 8
    count = height * LANES
    blocks_own = AGG_DEV // LANES
    dma = pltpu.SemaphoreType.DMA
    scratch = [pltpu.SMEM((height // SLOT_REFS, LANES), jnp.int32) for _ in range(SLOT_REFS)]
    scratch += [
        pltpu.SMEM((blocks_own, LANES), jnp.int32),
        pltpu.VMEM((height, LANES), jnp.int32),
        pltpu.VMEM((height, LANES), jnp.int32),
        pltpu.VMEM((blocks_own, LANES), jnp.int32),
        pltpu.VMEM((2 * blocks_own, LANES), jnp.float32),
        pltpu.VMEM((2, height, LANES), jnp.float32),
        pltpu.VMEM((pairs, FPA, 3, loads, width), jnp.float32),
        pltpu.VMEM(restriction.shape, jnp.float32),
        pltpu.VMEM(present.shape, jnp.int32),
        pltpu.VMEM(inverse.shape, jnp.float32),
        pltpu.VMEM(blocks.shape, jnp.float32),
        pltpu.VMEM(pattern.shape, jnp.int32),
        pltpu.VMEM((3, LANES, LANES), jnp.float32),
        pltpu.VMEM((pairs * devices * rows, LANES), jnp.float32),
        pltpu.VMEM((pairs, devices, rows, LANES), jnp.float32),
        pltpu.VMEM((AGG_DEV, LANES), jnp.float32),
        pltpu.VMEM((count, LANES), jnp.float32),
        pltpu.VMEM((planes * height, LANES), jnp.float32),
        pltpu.VMEM((planes * height, LANES), jnp.float32),
        pltpu.VMEM((planes, height, LANES), jnp.float32),
        pltpu.VMEM((2, planes, height + 16, LANES), jnp.float32),
        pltpu.VMEM((4, 3, 3, height, LANES), jnp.float32),
        pltpu.VMEM((steps, HALVES, 4, part_planes, LANES), jnp.float32),
        pltpu.VMEM((steps, HALVES, 4, part_planes, LANES), jnp.float32),
        pltpu.VMEM((HALVES, height, LANES), jnp.float32),
        pltpu.VMEM((HALVES, end_rows, LANES), jnp.float32),
        pltpu.VMEM((HALVES, end_rows, LANES), jnp.float32),
        pltpu.VMEM((pairs * devices * rows, LANES), jnp.float32),
        pltpu.VMEM(((pairs - 1) * devices * rows, LANES), jnp.float32),
        pltpu.VMEM((pairs - 1, 3, PAIR, LANES, LANES), jnp.float32),
        dma((pairs + 1,)),
        dma((pairs + 1,)),
        dma((5,)),
        dma((SLOT_REFS,)),
        dma,
        dma((pairs, 2)),
        dma((steps, HALVES, 4)),
        dma((steps, HALVES, 4)),
        dma((pairs,)),
        dma((pairs,)),
        dma((pairs,)),
    ]
    return pl.pallas_call(
        functools.partial(main_kernel, row_count, col_count, loads),
        in_specs=[spec_any()] * 7,
        out_specs=(spec_any(), spec_any(), spec_any()),
        out_shape=(
            jax.ShapeDtypeStruct((pairs - 1, 3, PAIR, LANES, LANES), jnp.float32),
            jax.ShapeDtypeStruct((devices, rows, LANES), jnp.float32),
            jax.ShapeDtypeStruct((planes * height, LANES), jnp.float32),
        ),
        scratch_shapes=scratch,
        compiler_params=pltpu.CompilerParams(vmem_limit_bytes=VMEM_LIMIT, collective_id=1, has_side_effects=True),
        name="correct",
    )(cells, residual, restriction, present, inverse, blocks, pattern)


def prolong_kernel(
    devices,
    values_hbm,
    last_hbm,
    restriction_hbm,
    pattern_hbm,
    planes_hbm,
    out_hbm,
    iterate_hbm,
    values,
    last,
    restriction,
    pattern,
    planes,
    out,
    restriction_sem,
    small_sem,
    out_sem,
    iterate_sem,
):
    final = values.shape[0] - 1
    parts = LANES // devices
    rows = last.shape[0] // devices
    loads = out.shape[1]
    blocks = AGG_DEV // LANES

    def slab(p):
        return pl.ds(pl.multiple_of(p * AGG_DEV, LANES), AGG_DEV)

    def restriction_copy(p):
        return pltpu.make_async_copy(restriction_hbm.at[:, :, slab(p)], restriction.at[:, :, slab(p)], restriction_sem.at[p])

    def out_copy(p):
        return pltpu.make_async_copy(out.at[:, :, slab(p)], out_hbm.at[:, :, slab(p)], out_sem.at[p])

    small = [
        pltpu.make_async_copy(pattern_hbm, pattern, small_sem.at[0]),
        pltpu.make_async_copy(values_hbm, values.at[pl.ds(0, final)], small_sem.at[1]),
        pltpu.make_async_copy(last_hbm, last, small_sem.at[3]),
        pltpu.make_async_copy(planes_hbm, planes, small_sem.at[2]),
    ]
    small[2].start()
    small[1].start()
    small[0].start()
    for p in range(FPA):
        restriction_copy(p).start()
    small[3].start()
    small[2].wait()
    for i in range(3):
        for half in range(PAIR):
            at = (i * PAIR + half) * parts
            pieces = [last[pl.ds(at + part, devices, stride=rows), :] for part in range(parts)]
            values[final, i, half] = jnp.concatenate(pieces, axis=0).T if parts > 1 else pieces[0].T
    small[0].wait()
    small[1].wait()

    def one(p, carry):
        restriction_copy(p).wait()
        for b in range(blocks):
            pair, half, block = b // (GROUP * PAIR), b // GROUP % PAIR, b % GROUP
            lanes = pl.ds(pl.multiple_of(p * AGG_DEV + b * LANES, LANES), LANES)
            present = pattern[pl.ds(p * blocks + b, 1), :].astype(jnp.float32)
            terms = [values[pair, i, half, block * loads : (block + 1) * loads, :] * present for i in range(3)]
            for j in range(3):
                total = restriction[0, j : j + 1, lanes] * terms[0]
                total = total + restriction[1, j : j + 1, lanes] * terms[1]
                out[j, :, lanes] = total + restriction[2, j : j + 1, lanes] * terms[2]
        out_copy(p).start()
        return carry

    lax.fori_loop(0, FPA, one, 0)
    small[3].wait()
    turned = [pltpu.make_async_copy(planes.at[i], iterate_hbm.at[:, i], iterate_sem.at[i]) for i in range(3)]
    for copy in turned:
        copy.start()
    for copy in turned:
        copy.wait()
    for p in range(FPA):
        out_copy(p).wait()


def prolong(values, last, restriction, pattern, planes, loads, height):
    pattern = pattern.reshape(-1, LANES)
    planes = planes.reshape(3, loads, height, LANES)
    devices = last.shape[0]
    last = last.reshape(-1, LANES)
    dma = pltpu.SemaphoreType.DMA
    shape = (3, loads, restriction.shape[2])
    out, iterate = pl.pallas_call(
        functools.partial(prolong_kernel, devices),
        in_specs=[spec_any()] * 5,
        out_specs=(spec_any(), spec_any()),
        out_shape=(
            jax.ShapeDtypeStruct(shape, jnp.float32),
            jax.ShapeDtypeStruct((loads, 3, height, LANES), jnp.float32),
        ),
        scratch_shapes=[
            pltpu.VMEM((values.shape[0] + 1,) + values.shape[1:], jnp.float32),
            pltpu.VMEM(last.shape, jnp.float32),
            pltpu.VMEM(restriction.shape, jnp.float32),
            pltpu.VMEM(pattern.shape, jnp.int32),
            pltpu.VMEM(planes.shape, jnp.float32),
            pltpu.VMEM(shape, jnp.float32),
            dma((FPA,)),
            dma((4,)),
            dma((FPA,)),
            dma((3,)),
        ],
        compiler_params=pltpu.CompilerParams(vmem_limit_bytes=VMEM_LIMIT),
        name="prolong",
    )(values, last, restriction, pattern, planes)
    return out.transpose(1, 0, 2), iterate


def body(
    fine_residual,
    restriction,
    restriction_pattern,
    cell_aggregate,
    block_inverse,
    off_blocks,
    operator_pattern,
):
    loads = fine_residual.shape[0]
    row_count = lax.axis_size("row")
    col_count = lax.axis_size("col")
    height = cell_aggregate.shape[0]
    values, last, planes = main(
        cell_aggregate,
        fine_residual,
        restriction,
        restriction_pattern,
        block_inverse,
        off_blocks,
        operator_pattern,
        row_count,
        col_count,
    )
    fine_correction, iterate = prolong(values, last, restriction, restriction_pattern, planes, loads, height)
    return (iterate, fine_correction)


def solution(mesh):
    in_specs = (
        P(None, None, ("row", "col")),
        P(None, None, ("row", "col")),
        P(("row", "col")),
        P("row", "col"),
        P(None, None, "row", "col"),
        P(None, None, None, "row", "col"),
        P(None, "row", "col"),
    )
    out_specs = (P(None, None, "row", "col"), P(None, None, ("row", "col")))
    return jax.shard_map(body, mesh=mesh, in_specs=in_specs, out_specs=out_specs, check_vma=False)
```
